16 devices in a mesh: dp: 4 (over z, y), tp: 4 (over x, core).
Axes of the slice: x: 2, y: 2, z: 2, core: 2. Of those that a mesh axis runs over, the one named last changes fastest.
Arguments:
- irreps: bfloat16 [1024, 25, 128], P('dp', None, 'tp')
- norm_gain: float32 [5, 128], P(None, 'tp')
- w_up: bfloat16 [5, 128, 512], P(None, None, 'tp')
- w_gate: bfloat16 [128, 512], P(None, 'tp')
- w_down: bfloat16 [5, 512, 128], P(None, 'tp')
- to_grid: float32 [25, 196], replicated
- from_grid: float32 [196, 24], replicated
- grad_out: bfloat16 [1024, 25, 128], P('dp', None, 'tp')
Outputs:
- output 1: bfloat16 [1024, 25, 128], P('dp', None, 'tp')
- output 2: bfloat16 [1024, 25, 128], P('dp', None, 'tp')
- output 3: bfloat16 [5, 128, 512], P(None, None, 'tp')
- output 4: bfloat16 [128, 512], P(None, 'tp')
- output 5: bfloat16 [5, 512, 128], P(None, 'tp')
All inputs are finite; a program needn't handle non-finite values.
Results may differ from the reference program's by a relative error of at most 0.0126671.
Values are sent between devices in bfloat16 or wider.
A program may use at most 1 GiB of HBM per device.

```python
import math
import jax
import jax.numpy as jnp
from jax import lax

N_NODES = 1024
CHANNELS = 128
HIDDEN = 512
DEG_MAX = 4
GRID_PTS = 196

DEGREES = DEG_MAX + 1
COEFS = DEGREES * DEGREES
ROW_BLOCK = math.gcd(N_NODES, 128)
NORM_EPS = 1e-5


def setup_inputs(seed: int = 0) -> dict:
    key_list = jax.random.split(jax.random.key(seed), 11)
    chan_pos = jnp.arange(CHANNELS, dtype=jnp.float32) / CHANNELS
    chan_scale = jnp.exp(2.4 * (chan_pos - 0.5) + 0.3 * jax.random.normal(key_list[0], (CHANNELS,)))
    node_scale = jnp.exp(0.4 * jax.random.normal(key_list[1], (N_NODES, 1, 1)))
    scalar_row = (jnp.arange(COEFS) == 0).astype(jnp.float32)[:, None]
    offsets = 0.8 * jax.random.normal(key_list[2], (CHANNELS,))
    noise_draw = jax.random.normal(key_list[3], (N_NODES, COEFS, CHANNELS))
    irreps = node_scale * chan_scale * (noise_draw + scalar_row * offsets)
    norm_gain = 0.6 + 0.8 * jax.random.uniform(key_list[4], (DEGREES, CHANNELS))
    w_up = jax.random.normal(key_list[5], (DEGREES, CHANNELS, HIDDEN)) * CHANNELS ** -0.5
    w_gate = jax.random.normal(key_list[6], (CHANNELS, HIDDEN)) * CHANNELS ** -0.5
    w_down = jax.random.normal(key_list[7], (DEGREES, HIDDEN, CHANNELS)) * HIDDEN ** -0.5
    to_grid = jax.random.normal(key_list[8], (COEFS, GRID_PTS)) * COEFS ** -0.5
    from_grid = jax.random.normal(key_list[9], (GRID_PTS, COEFS - 1)) * GRID_PTS ** -0.5
    grad_out = jax.random.normal(key_list[10], (N_NODES, COEFS, CHANNELS))
    return {'irreps': irreps.astype(jnp.bfloat16), 'norm_gain': norm_gain, 'w_up': w_up.astype(jnp.bfloat16), 'w_gate': w_gate.astype(jnp.bfloat16), 'w_down': w_down.astype(jnp.bfloat16), 'to_grid': to_grid, 'from_grid': from_grid, 'grad_out': grad_out.astype(jnp.bfloat16)}


def expand_rows(per_degree):
    return jnp.concatenate([jnp.broadcast_to(per_degree[degree:degree + 1], (2 * degree + 1,) + per_degree.shape[1:]) for degree in range(per_degree.shape[0])], axis=0)


def block_forward(x_blk, norm_gain, up_f, gate_f, down_f, grid_in, grid_back):
    x_f = x_blk.astype(jnp.float32)
    scalar = x_f[:, 0, :]
    mean_s = jnp.mean(scalar, axis=-1, keepdims=True)
    centered = scalar - mean_s
    var_s = jnp.mean(centered * centered, axis=-1, keepdims=True)
    vector = x_f[:, 1:, :]
    mean_sq = jnp.mean(vector * vector, axis=(1, 2), keepdims=True)
    normed = jnp.concatenate([(centered * lax.rsqrt(var_s + NORM_EPS))[:, None, :], vector * lax.rsqrt(mean_sq + NORM_EPS)], axis=1)
    normed = (normed * expand_rows(norm_gain)).astype(jnp.bfloat16).astype(jnp.float32)
    hidden_act = jnp.einsum('nkc,kch->nkh', normed, expand_rows(up_f)).astype(jnp.bfloat16).astype(jnp.float32)
    pre_gate = jnp.einsum('nc,ch->nh', normed[:, 0, :], gate_f).astype(jnp.bfloat16).astype(jnp.float32)
    gate_val = jax.nn.silu(pre_gate).astype(jnp.bfloat16)
    pre_grid = jnp.einsum('nkh,kg->ngh', hidden_act, grid_in).astype(jnp.bfloat16).astype(jnp.float32)
    grid_val = jax.nn.silu(pre_grid).astype(jnp.bfloat16).astype(jnp.float32)
    back_proj = jnp.einsum('ngh,gk->nkh', grid_val, grid_back).astype(jnp.bfloat16)
    mixed_act = jnp.concatenate([gate_val[:, None, :], back_proj], axis=1).astype(jnp.float32)
    ffn_delta = jnp.einsum('nkh,khc->nkc', mixed_act, expand_rows(down_f))
    return (x_f + ffn_delta).astype(jnp.bfloat16)


def reference(irreps, norm_gain, w_up, w_gate, w_down, to_grid, from_grid, grad_out):
    up_f = w_up.astype(jnp.float32)
    gate_f = w_gate.astype(jnp.float32)
    down_f = w_down.astype(jnp.float32)
    grid_in = to_grid.astype(jnp.bfloat16).astype(jnp.float32)
    grid_back = from_grid.astype(jnp.bfloat16).astype(jnp.float32)
    blk_count = N_NODES // ROW_BLOCK
    x_blocks = irreps.reshape(blk_count, ROW_BLOCK, COEFS, CHANNELS)
    g_blocks = grad_out.reshape(blk_count, ROW_BLOCK, COEFS, CHANNELS)

    def scan_step(grad_sums, blk_pair):
        def local_fn(x_in, up_in, gate_in, down_in):
            return block_forward(x_in, norm_gain, up_in, gate_in, down_in, grid_in, grid_back)
        out_blk, pull_back = jax.vjp(local_fn, blk_pair[0], up_f, gate_f, down_f)
        dx_blk, d_up, d_gate, d_down = pull_back(blk_pair[1])
        new_sums = (grad_sums[0] + d_up, grad_sums[1] + d_gate, grad_sums[2] + d_down)
        return new_sums, (out_blk, dx_blk)

    init_sums = (jnp.zeros_like(up_f), jnp.zeros_like(gate_f), jnp.zeros_like(down_f))
    total_sums, (out_blocks, dx_blocks) = lax.scan(scan_step, init_sums, (x_blocks, g_blocks))
    out_irreps = out_blocks.reshape(N_NODES, COEFS, CHANNELS)
    d_irreps = dx_blocks.reshape(N_NODES, COEFS, CHANNELS)
    return (out_irreps, d_irreps, total_sums[0].astype(jnp.bfloat16), total_sums[1].astype(jnp.bfloat16), total_sums[2].astype(jnp.bfloat16))
```

```python
import functools
import math
import jax
import jax.numpy as jnp
from jax import lax
from jax.experimental import pallas as pl
from jax.experimental.pallas import tpu as pltpu
from jax.sharding import PartitionSpec as P

NORM_EPS = 1e-5
F32 = jnp.float32
BF16 = jnp.bfloat16
MESH = pl.DeviceIdType.MESH
LANES = 128
SUB = 8
KPAD = 256


def mm(lhs, rhs):
    return jnp.dot(lhs, rhs, preferred_element_type=F32)


def mm_nt(lhs, rhs):
    return lax.dot_general(lhs, rhs, (((1,), (1,)), ((), ())), preferred_element_type=F32)


def degree_span(degree):
    return range(degree * degree, (degree + 1) * (degree + 1))


def lane_cat(ref, chunk, degree):
    parts = [ref[chunk, coef] for coef in degree_span(degree)]
    return parts[0] if len(parts) == 1 else jnp.concatenate(parts, axis=1)


def pair_rows(first, second):
    groups = first.shape[0] // SUB
    shape = (groups, SUB, first.shape[1])
    return jnp.concatenate([first.reshape(shape), second.reshape(shape)], axis=1).astype(BF16)


def split_coefs(per_degree):
    out = []
    for degree, value in enumerate(per_degree):
        out += [value[:, LANES * j:LANES * (j + 1)] for j in range(2 * degree + 1)]
    return out


def rounded(value):
    return value.astype(BF16).astype(F32)


def iota2(shape, axis):
    return lax.broadcasted_iota(jnp.int32, shape, axis)


def ones_where(cond):
    return jnp.where(cond, 1.0, 0.0).astype(BF16)


def dp_peer(hop):
    dp = lax.axis_index('dp')
    zpos, ypos = dp // 2, dp % 2
    if hop % 2:
        ypos = 1 - ypos
    if hop // 2:
        zpos = 1 - zpos
    return zpos * 2 + ypos


def tp_peer(hop):
    tp = lax.axis_index('tp')
    xpos, core = tp // 2, tp % 2
    if hop % 2:
        core = 1 - core
    if hop // 2:
        xpos = 1 - xpos
    return xpos * 2 + core


def chan_rows(tp, chan_loc):
    return pl.ds(pl.multiple_of(tp * chan_loc, chan_loc), chan_loc)


def build_grid_mats(to_ref, fromt_ref, up_mat, dgrid_mat, z_mat, dh_mat, blk_pts):
    coefs, points = to_ref.shape
    vecs = fromt_ref.shape[0]
    blk_rows = blk_pts * SUB
    to_b = to_ref[...].astype(BF16)
    from_b = fromt_ref[...].astype(BF16)

    def spread(count, shape, axis):
        return ones_where(iota2(shape, axis) // SUB == iota2(shape, 1 - axis))

    to_cols = lax.dot_general(to_b, spread(coefs, (coefs, KPAD), 1), (((0,), (0,)), ((), ())), preferred_element_type=F32)
    from_cols = lax.dot_general(from_b, spread(vecs, (vecs, KPAD), 1), (((0,), (0,)), ((), ())), preferred_element_type=F32)
    to_cols = (to_cols * 0.5).astype(BF16)
    from_cols = (from_cols * 0.5).astype(BF16)
    to_rows = mm(spread(coefs, (dh_mat.shape[1], coefs), 0), to_b).astype(BF16)
    from_rows = mm(spread(vecs, (z_mat.shape[1], vecs), 0), from_b).astype(BF16)

    def diagonal(value):
        same = iota2(value.shape, 0) % SUB == iota2(value.shape, 1) % SUB
        return jnp.where(same, value, 0.0).astype(BF16)

    def blk_step(blk, carry):
        first = blk * blk_pts
        shape = (blk_rows, points)
        pick = ones_where(iota2(shape, 0) // SUB + first == iota2(shape, 1))
        shape = (points, KPAD)
        col = iota2(shape, 1)
        pick_t = ones_where((col // SUB + first == iota2(shape, 0)) & (col < blk_rows))
        up_mat[blk] = diagonal(mm(pick, to_cols))
        dgrid_mat[blk] = diagonal(mm(pick, from_cols))
        z_mat[blk] = diagonal(mm(from_rows, pick_t))
        dh_mat[blk] = diagonal(mm(to_rows, pick_t))
        return carry

    lax.fori_loop(0, points // blk_pts, blk_step, 0)


def kernel(dims, x_ref, g_ref, gain_ref, up_ref, gate_ref, down_ref, to_ref, fromt_ref,
           out_ref, dx_ref, dup_ref, dgate_ref, ddown_ref,
           xfull, gfull, nfull, gain_rx, gain_cols, up_t, down_t, gate_t,
           up_mat, dgrid_mat, z_mat, dh_mat, ybuf, dmbuf, dgbuf, dm_zero, mbuf, dhbuf, dpg_buf,
           stat_buf, part, rs1, rs2_src, rs2, back_src, back_rx, wgrad, wgrad_rx, wsum, wfull,
           ag_ss, ag_rs, gain_ss, gain_rs, rs1_ss, rs1_rs, rs2_ss, rs2_rs, back_ss, back_rs, w1_ss, w1_rs, w2_ss, w2_rs):
    coefs, chan_loc, _ = x_ref.shape
    degrees = gain_ref.shape[0]
    channels = chan_loc * 4
    vec_count = channels * (coefs - 1)
    hidden = gate_ref.shape[1]
    chunks = dims['chunks']
    blk_count = up_mat.shape[0]
    blk_rows = up_mat.shape[1]
    steps = hidden // SUB // 2
    quarter = wgrad.shape[0] // 4
    me = lax.axis_index('tp')
    my_dp = lax.axis_index('dp')
    sources = (g_ref, x_ref)
    fulls = (gfull, xfull)
    grad, feat = 0, 1
    dxs, outs = 0, 1
    copies = {}

    def send(key, src, dst, ssem, rsem, axis, peer):
        copy = pltpu.make_async_remote_copy(src_ref=src, dst_ref=dst, send_sem=ssem, recv_sem=rsem, device_id={axis: peer}, device_id_type=MESH)
        copy.start()
        copies[key] = copy

    def lanes_of(chunk):
        return pl.ds(chunk * LANES, LANES)

    barrier = pltpu.get_barrier_semaphore()
    for hop in (1, 2, 3):
        pl.semaphore_signal(barrier, inc=1, device_id={'tp': tp_peer(hop)}, device_id_type=MESH)
        pl.semaphore_signal(barrier, inc=1, device_id={'dp': dp_peer(hop)}, device_id_type=MESH)
    pl.semaphore_wait(barrier, 6)

    for hop in (1, 2, 3):
        send(('gain', hop), gain_ref, gain_rx.at[hop - 1], gain_ss.at[hop - 1], gain_rs.at[hop - 1], 'tp', tp_peer(hop))
    for chunk in range(chunks):
        for arr in (grad, feat):
            for hop in (2, 1):
                send(('ag', arr, chunk, hop), sources[arr].at[:, :, lanes_of(chunk)], fulls[arr].at[chunk, :, chan_rows(me, chan_loc), :],
                     ag_ss.at[arr, chunk, hop - 1], ag_rs.at[arr, chunk, hop - 1], 'tp', tp_peer(hop))

    def relay(arr, chunk):
        copies[('ag', arr, chunk, 2)].wait_recv()
        block = fulls[arr].at[chunk, :, chan_rows(tp_peer(2), chan_loc), :]
        send(('ag', arr, chunk, 3), block, block, ag_ss.at[arr, chunk, 2], ag_rs.at[arr, chunk, 2], 'tp', tp_peer(1))

    def gathered(arr, chunk):
        copies[('ag', arr, chunk, 1)].wait_recv()
        copies[('ag', arr, chunk, 3)].wait_recv()

    for chunk in range(chunks):
        for arr in (grad, feat):
            fulls[arr][chunk, :, chan_rows(me, chan_loc), :] = sources[arr][:, :, chunk * LANES:(chunk + 1) * LANES]
    build_grid_mats(to_ref, fromt_ref, up_mat, dgrid_mat, z_mat, dh_mat, dims['blk_pts'])
    for degree in range(degrees):
        up_t[degree] = up_ref[degree].astype(F32).T.astype(BF16)
        down_t[degree] = down_ref[degree].astype(F32).T.astype(BF16)
    gate_t[...] = gate_ref[...].astype(F32).T.astype(BF16)
    for buf in (ybuf, dmbuf):
        tail = 192
        buf[:, tail:, :] = jnp.zeros((buf.shape[0], KPAD - tail, LANES), BF16)
    wgrad[...] = jnp.zeros_like(wgrad)
    back_src[...] = jnp.zeros_like(back_src)

    def gain_block(tp, rows):
        eye = iota2((chan_loc, chan_loc), 0) == iota2((chan_loc, chan_loc), 1)
        for degree in range(degrees):
            col = jnp.sum(jnp.where(eye, rows[degree:degree + 1, :], 0.0), axis=1, keepdims=True)
            gain_cols[degree, chan_rows(tp, chan_loc), :] = jnp.broadcast_to(col, (chan_loc, LANES))

    gain_block(me, gain_ref[...])

    def grad_part(chunk):
        d_mixed = split_coefs([mm(down_ref[degree], lane_cat(gfull, chunk, degree)) for degree in range(degrees)])
        dm_zero[...] = rounded(d_mixed[0])
        for pair in range((coefs - 1) // 2):
            dmbuf[:, 16 * pair:16 * pair + 16, :] = pair_rows(d_mixed[2 * pair + 1], d_mixed[2 * pair + 2])

        def step(idx, carry):
            rhs = jnp.concatenate([dmbuf[2 * idx], dmbuf[2 * idx + 1]], axis=1)
            for blk in range(blk_count):
                dgbuf[idx, blk] = mm(dgrid_mat[blk], rhs).astype(BF16)
            return carry

        lax.fori_loop(0, steps, step, 0)

    def normalize(chunk):
        scalar = xfull[chunk, 0].astype(F32)
        mean = jnp.sum(scalar, axis=0, keepdims=True) / channels
        centered = scalar - mean
        inv_s = lax.rsqrt(jnp.sum(centered * centered, axis=0, keepdims=True) / channels + NORM_EPS)
        squares = jnp.zeros((channels, LANES), F32)
        for coef in range(1, coefs):
            vec = xfull[chunk, coef].astype(F32)
            squares = squares + vec * vec
        inv_v = lax.rsqrt(jnp.sum(squares, axis=0, keepdims=True) / vec_count + NORM_EPS)
        stat_buf[chunk, 0:1, :] = mean
        stat_buf[chunk, 1:2, :] = inv_s
        stat_buf[chunk, 2:3, :] = inv_v
        nfull[chunk, 0] = (centered * inv_s * gain_cols[0]).astype(BF16)
        for degree in range(1, degrees):
            for coef in degree_span(degree):
                nfull[chunk, coef] = (xfull[chunk, coef].astype(F32) * inv_v * gain_cols[degree]).astype(BF16)

    def hidden_part(chunk):
        hid = split_coefs([mm(up_t[degree], lane_cat(nfull, chunk, degree)) for degree in range(degrees)])
        hid.append(jnp.zeros_like(hid[0]))
        for pair in range((coefs + 1) // 2):
            ybuf[:, 16 * pair:16 * pair + 16, :] = pair_rows(hid[2 * pair], hid[2 * pair + 1])
        half = rounded(mm(gate_t[...], nfull[chunk, 0])) * 0.5
        tan = jnp.tanh(half)
        wide = 1.0 + tan
        act = half * wide
        mbuf[chunk, 0] = act.astype(BF16)
        dpg_buf[chunk] = (dm_zero[...] * (0.5 * (wide + act * (1.0 - tan)))).astype(BF16)

    def grid_step(chunk, idx, carry):
        rhs = jnp.concatenate([ybuf[2 * idx], ybuf[2 * idx + 1]], axis=1)
        z_sum = None
        pad = jnp.zeros((KPAD - blk_rows, 2 * LANES), BF16)
        for blk in range(blk_count):
            half = rounded(mm(up_mat[blk], rhs))
            tan = jnp.tanh(half)
            wide = 1.0 + tan
            act = half * wide
            d_pre = dgbuf[idx, blk].astype(F32) * (wide + act * (1.0 - tan))
            z_add = mm(z_mat[blk], jnp.concatenate([act.astype(BF16), pad], axis=0))
            h_add = mm(dh_mat[blk], jnp.concatenate([d_pre.astype(BF16), pad], axis=0))
            z_sum, h_sum = (z_add, h_add) if z_sum is None else (z_sum + z_add, h_sum + h_add)
        rows = pl.ds(pl.multiple_of(16 * idx, 16), 16)

        def by_coef(value, count):
            value = value[:count * SUB].reshape(count, SUB, 2 * LANES)
            return jnp.concatenate([value[:, :, :LANES], value[:, :, LANES:]], axis=1).astype(BF16)

        mbuf[chunk, 1:coefs, rows, :] = by_coef(z_sum, coefs - 1)
        dhbuf[chunk, :, rows, :] = by_coef(h_sum, coefs)
        return carry

    def grid_part(chunk, first, last):
        lax.fori_loop(first, last, functools.partial(grid_step, chunk), 0)

    def weight_grads(chunk):
        for degree in range(degrees):
            rows = pl.ds(degree * channels, channels)
            wgrad[rows, :] += mm_nt(lane_cat(nfull, chunk, degree), lane_cat(dhbuf, chunk, degree))
            rows = pl.ds((degrees + 1) * channels + degree * hidden, hidden)
            wgrad[rows, :] += mm_nt(lane_cat(mbuf, chunk, degree), lane_cat(gfull, chunk, degree))
        rows = pl.ds(degrees * channels, channels)
        wgrad[rows, :] += mm_nt(nfull[chunk, 0], dpg_buf[chunk])

    def store_part(arr, chunk, per_degree):
        for coef, value in enumerate(split_coefs(per_degree)):
            part[arr, chunk, coef] = value.astype(BF16)

    def input_grads(chunk):
        per_degree = [mm(up_ref[degree], lane_cat(dhbuf, chunk, degree)) for degree in range(degrees)]
        per_degree[0] = per_degree[0] + mm(gate_ref[...], dpg_buf[chunk])
        store_part(dxs, chunk, per_degree)

    def outputs(chunk):
        store_part(outs, chunk, [mm(down_t[degree], lane_cat(mbuf, chunk, degree)) for degree in range(degrees)])

    def scatter_core(arr, chunk):
        for chip in (0, 1):
            rows = chan_rows(2 * chip + 1 - me % 2, chan_loc)
            send(('rs1', arr, chunk, chip), part.at[arr, chunk, :, rows, :], rs1.at[arr, chunk, chip],
                 rs1_ss.at[arr, chunk, chip], rs1_rs.at[arr, chunk, chip], 'tp', tp_peer(1))

    def chip_sum(arr, chunk, chip):
        own = part[arr, chunk, :, chan_rows(2 * chip + me % 2, chan_loc), :].astype(F32)
        return own + rs1[arr, chunk, chip].astype(F32)

    def scatter_chip(arr, chunk):
        for chip in (0, 1):
            copies[('rs1', arr, chunk, chip)].wait_recv()
        rs2_src[arr, chunk] = chip_sum(arr, chunk, 1 - me // 2).astype(BF16)
        send(('rs2', arr, chunk), rs2_src.at[arr, chunk], rs2.at[arr, chunk], rs2_ss.at[arr, chunk], rs2_rs.at[arr, chunk], 'tp', tp_peer(2))

    def scattered(arr, chunk):
        copies[('rs2', arr, chunk)].wait_recv()
        return chip_sum(arr, chunk, me // 2) + rs2[arr, chunk].astype(F32)

    def own_x(chunk):
        return x_ref[:, :, chunk * LANES:(chunk + 1) * LANES].astype(F32)

    def finish_out(chunk):
        out_ref[:, :, chunk * LANES:(chunk + 1) * LANES] = (own_x(chunk) + scattered(outs, chunk)).astype(BF16)

    def own_gain(degree):
        return gain_cols[degree, chan_rows(me, chan_loc), :]

    def back_stats(chunk):
        x_own = own_x(chunk)
        d_norm = rounded(scattered(dxs, chunk))
        rs2[dxs, chunk] = d_norm.astype(BF16)
        d_hat = d_norm[0] * own_gain(0)
        hat = (x_own[0] - stat_buf[chunk, 0:1, :]) * stat_buf[chunk, 1:2, :]
        back_src[chunk, 0:1, :] = jnp.sum(d_hat, axis=0, keepdims=True)
        back_src[chunk, 1:2, :] = jnp.sum(d_hat * hat, axis=0, keepdims=True)
        total = jnp.zeros((chan_loc, LANES), F32)
        for degree in range(1, degrees):
            for coef in degree_span(degree):
                total = total + d_norm[coef] * own_gain(degree) * x_own[coef]
        back_src[chunk, 2:3, :] = jnp.sum(total, axis=0, keepdims=True)
        for hop in (2, 3, 1):
            send(('back', chunk, hop), back_src.at[chunk], back_rx.at[chunk, hop - 1], back_ss.at[chunk, hop - 1], back_rs.at[chunk, hop - 1], 'tp', tp_peer(hop))

    def finish_dx(chunk):
        for hop in (1, 2, 3):
            copies[('back', chunk, hop)].wait_recv()
        sums = (back_src[chunk] + back_rx[chunk, 0]) + (back_rx[chunk, 1] + back_rx[chunk, 2])
        mean, inv_s, inv_v = (stat_buf[chunk, j:j + 1, :] for j in range(3))
        lanes = slice(chunk * LANES, (chunk + 1) * LANES)
        hat = (x_ref[0, :, lanes].astype(F32) - mean) * inv_s
        d_hat = rs2[dxs, chunk, 0].astype(F32) * own_gain(0)
        d_scalar = inv_s * (d_hat - sums[0:1] / channels - hat * (sums[1:2] / channels))
        dx_ref[0, :, lanes] = (d_scalar + g_ref[0, :, lanes].astype(F32)).astype(BF16)
        scale = (inv_v * inv_v * inv_v) * (sums[2:3] / vec_count)
        for degree in range(1, degrees):
            for coef in degree_span(degree):
                d_hat = rs2[dxs, chunk, coef].astype(F32) * own_gain(degree)
                d_vec = inv_v * d_hat - x_ref[coef, :, lanes].astype(F32) * scale
                dx_ref[coef, :, lanes] = (d_vec + g_ref[coef, :, lanes].astype(F32)).astype(BF16)

    def quarter_rows(dp):
        return pl.ds(pl.multiple_of(dp * quarter, 16), quarter)

    def wgrad_scatter():
        for hop in (3, 1, 2):
            send(('w1', hop), wgrad.at[quarter_rows(dp_peer(hop))], wgrad_rx.at[hop - 1], w1_ss.at[hop - 1], w1_rs.at[hop - 1], 'dp', dp_peer(hop))

    def wgrad_reduce():
        for hop in (1, 2, 3):
            copies[('w1', hop)].wait_recv()
        total = (wgrad[quarter_rows(my_dp), :] + wgrad_rx[0]) + (wgrad_rx[1] + wgrad_rx[2])
        wsum[...] = total.astype(BF16)
        wfull[quarter_rows(my_dp), :] = wsum[...]
        for hop in (3, 1, 2):
            send(('w2', hop), wsum, wfull.at[quarter_rows(my_dp)], w2_ss.at[hop - 1], w2_rs.at[hop - 1], 'dp', dp_peer(hop))

    def wgrad_finish():
        for hop in (1, 2, 3):
            copies[('w2', hop)].wait_recv()
        dup_ref[...] = wfull[:degrees * channels, :]
        dgate_ref[...] = wfull[degrees * channels:(degrees + 1) * channels, :]
        ddown_ref[...] = wfull[(degrees + 1) * channels:, :]

    relay(grad, 0)
    for hop in (1, 2, 3):
        copies[('gain', hop)].wait_recv()
        gain_block(tp_peer(hop), gain_rx[hop - 1])
    gathered(grad, 0)
    grad_part(0)
    relay(feat, 0)
    gathered(feat, 0)
    normalize(0)
    hidden_part(0)
    grid_part(0, 0, steps // 2)
    relay(grad, 1)
    grid_part(0, steps // 2, steps)
    weight_grads(0)
    input_grads(0)
    scatter_core(dxs, 0)
    outputs(0)
    scatter_core(outs, 0)
    relay(feat, 1)
    scatter_chip(dxs, 0)
    gathered(grad, 1)
    grad_part(1)
    scatter_chip(outs, 0)
    gathered(feat, 1)
    normalize(1)
    hidden_part(1)
    grid_part(1, 0, steps)
    weight_grads(1)
    wgrad_scatter()
    input_grads(1)
    scatter_core(dxs, 1)
    outputs(1)
    scatter_chip(dxs, 1)
    scatter_core(outs, 1)
    back_stats(0)
    scatter_chip(outs, 1)
    finish_out(0)
    finish_dx(0)
    wgrad_reduce()
    back_stats(1)
    finish_out(1)
    finish_dx(1)
    wgrad_finish()
    for copy in copies.values():
        copy.wait_send()


def solution(mesh):
    act_spec = P('dp', None, 'tp')
    in_specs = (act_spec, P(None, 'tp'), P(None, None, 'tp'), P(None, 'tp'), P(None, 'tp', None), P(None, None), P(None, None), act_spec)
    out_specs = (act_spec, act_spec, P(None, None, 'tp'), P(None, 'tp'), P(None, 'tp', None))

    def local_step(x_loc, gain_loc, up_loc, gate_loc, down_loc, to_grid, from_grid, grad_loc):
        nodes, coefs, chan_loc = x_loc.shape
        degrees, channels, hidden = up_loc.shape
        points = to_grid.shape[1]
        blk_pts = 28
        blks = points // blk_pts
        chunks = nodes // LANES
        groups = hidden // SUB
        w_rows = degrees * channels + channels + degrees * hidden
        dma = pltpu.SemaphoreType.DMA

        def vm(*shape, dtype=BF16):
            return pltpu.VMEM(shape, dtype)

        full = (chunks, coefs, channels, LANES)
        scratch = [
            vm(*full), vm(*full), vm(*full),
            vm(3, degrees, chan_loc, dtype=F32), vm(degrees, channels, LANES, dtype=F32),
            vm(degrees, hidden, channels), vm(degrees, channels, hidden), vm(hidden, channels),
            vm(blks, blk_pts * SUB, KPAD), vm(blks, blk_pts * SUB, KPAD), vm(blks, (coefs - 1) * SUB, KPAD), vm(blks, (coefs + 1) * SUB, KPAD),
            vm(groups, KPAD, LANES), vm(groups, KPAD, LANES), vm(groups // 2, blks, blk_pts * SUB, 2 * LANES),
            vm(hidden, LANES, dtype=F32), vm(chunks, coefs, hidden, LANES), vm(chunks, coefs, hidden, LANES), vm(chunks, hidden, LANES),
            vm(chunks, SUB, LANES, dtype=F32),
            vm(2, *full), vm(2, chunks, 2, coefs, chan_loc, LANES), vm(2, chunks, coefs, chan_loc, LANES), vm(2, chunks, coefs, chan_loc, LANES),
            vm(chunks, SUB, LANES, dtype=F32), vm(chunks, 3, SUB, LANES, dtype=F32),
            vm(w_rows, hidden, dtype=F32), vm(3, w_rows // 4, hidden, dtype=F32), vm(w_rows // 4, hidden), vm(w_rows, hidden),
            dma((2, chunks, 3)), dma((2, chunks, 3)), dma((3,)), dma((3,)),
            dma((2, chunks, 2)), dma((2, chunks, 2)), dma((2, chunks)), dma((2, chunks)),
            dma((chunks, 3)), dma((chunks, 3)), dma((3,)), dma((3,)), dma((3,)), dma((3,)),
        ]
        vmem = pl.BlockSpec(memory_space=pltpu.VMEM)
        act = jax.ShapeDtypeStruct((coefs, chan_loc, nodes), BF16)
        out_t, dx_t, d_up, d_gate, d_down = pl.pallas_call(
            functools.partial(kernel, {'chunks': chunks, 'blk_pts': blk_pts}),
            out_shape=(act, act, jax.ShapeDtypeStruct((degrees * channels, hidden), BF16), jax.ShapeDtypeStruct((channels, hidden), BF16), jax.ShapeDtypeStruct((degrees * hidden, channels), BF16)),
            in_specs=[vmem] * 8,
            out_specs=(vmem,) * 5,
            scratch_shapes=scratch,
            compiler_params=pltpu.CompilerParams(collective_id=0, has_side_effects=True, vmem_limit_bytes=60 * 1024 * 1024),
            name='s2_ffn',
        )(x_loc.transpose(1, 2, 0), grad_loc.transpose(1, 2, 0), gain_loc, up_loc, gate_loc, down_loc, to_grid, from_grid.T)
        return (out_t.transpose(2, 0, 1), dx_t.transpose(2, 0, 1), d_up.reshape(degrees, channels, hidden), d_gate, d_down.reshape(degrees, hidden, channels))

    return jax.shard_map(local_step, mesh=mesh, in_specs=in_specs, out_specs=out_specs, check_vma=False)
```

```python
import functools
import math
import jax
import jax.numpy as jnp
from jax import lax
from jax.experimental import pallas as pl
from jax.experimental.pallas import tpu as pltpu
from jax.sharding import PartitionSpec as P

NORM_EPS = 1e-5
F32 = jnp.float32
BF16 = jnp.bfloat16
MESH = pl.DeviceIdType.MESH
LANES = 128
SUB = 8
KPAD = 256


def mm(lhs, rhs):
    return jnp.dot(lhs, rhs, preferred_element_type=F32)


def mm_nt(lhs, rhs):
    return lax.dot_general(lhs, rhs, (((1,), (1,)), ((), ())), preferred_element_type=F32)


def degree_span(degree):
    return range(degree * degree, (degree + 1) * (degree + 1))


def lane_cat(ref, chunk, degree):
    parts = [ref[chunk, coef] for coef in degree_span(degree)]
    return parts[0] if len(parts) == 1 else jnp.concatenate(parts, axis=1)


def pair_rows(first, second):
    groups = first.shape[0] // SUB
    shape = (groups, SUB, first.shape[1])
    return jnp.concatenate([first.reshape(shape), second.reshape(shape)], axis=1).astype(BF16)


def split_coefs(per_degree):
    out = []
    for degree, value in enumerate(per_degree):
        out += [value[:, LANES * j:LANES * (j + 1)] for j in range(2 * degree + 1)]
    return out


def rounded(value):
    return value.astype(BF16).astype(F32)


def iota2(shape, axis):
    return lax.broadcasted_iota(jnp.int32, shape, axis)


def ones_where(cond):
    return jnp.where(cond, 1.0, 0.0).astype(BF16)


def dp_peer(hop):
    dp = lax.axis_index('dp')
    zpos, ypos = dp // 2, dp % 2
    if hop % 2:
        ypos = 1 - ypos
    if hop // 2:
        zpos = 1 - zpos
    return zpos * 2 + ypos


def tp_peer(hop):
    tp = lax.axis_index('tp')
    xpos, core = tp // 2, tp % 2
    if hop % 2:
        core = 1 - core
    if hop // 2:
        xpos = 1 - xpos
    return xpos * 2 + core


def chan_rows(tp, chan_loc):
    return pl.ds(pl.multiple_of(tp * chan_loc, chan_loc), chan_loc)


def load_wide(ref, index):
    return jnp.concatenate([ref[index + (0,)], ref[index + (1,)]], axis=1)


def store_wide(ref, index, value):
    ref[index + (0,)] = value[:, :LANES]
    ref[index + (1,)] = value[:, LANES:]


def build_grid_mats(to_ref, fromt_ref, up_mat, dgrid_mat, z_mat, dh_mat, blk_pts):
    coefs, points = to_ref.shape
    vecs = fromt_ref.shape[0]
    blk_rows = blk_pts * SUB
    to_b = to_ref[...].astype(BF16)
    from_b = fromt_ref[...].astype(BF16)

    def spread(count, shape, axis):
        return ones_where(iota2(shape, axis) // SUB == iota2(shape, 1 - axis))

    to_cols = lax.dot_general(to_b, spread(coefs, (coefs, KPAD), 1), (((0,), (0,)), ((), ())), preferred_element_type=F32)
    from_cols = lax.dot_general(from_b, spread(vecs, (vecs, KPAD), 1), (((0,), (0,)), ((), ())), preferred_element_type=F32)
    to_cols = (to_cols * 0.5).astype(BF16)
    from_cols = (from_cols * 0.5).astype(BF16)
    to_rows = mm(spread(coefs, (dh_mat.shape[2], coefs), 0), to_b).astype(BF16)
    from_rows = mm(spread(vecs, (z_mat.shape[2], vecs), 0), from_b).astype(BF16)

    def diagonal(value):
        same = iota2(value.shape, 0) % SUB == iota2(value.shape, 1) % SUB
        return jnp.where(same, value, 0.0).astype(BF16)

    def blk_step(blk, carry):
        first = blk * blk_pts
        shape = (blk_rows, points)
        pick = ones_where(iota2(shape, 0) // SUB + first == iota2(shape, 1))
        shape = (points, KPAD)
        col = iota2(shape, 1)
        pick_t = ones_where((col // SUB + first == iota2(shape, 0)) & (col < blk_rows))
        store_wide(up_mat, (blk,), diagonal(mm(pick, to_cols)))
        store_wide(dgrid_mat, (blk,), diagonal(mm(pick, from_cols)))
        store_wide(z_mat, (blk,), diagonal(mm(from_rows, pick_t)))
        store_wide(dh_mat, (blk,), diagonal(mm(to_rows, pick_t)))
        return carry

    lax.fori_loop(0, points // blk_pts, blk_step, 0)


def kernel(dims, x_ref, g_ref, gain_ref, up_ref, gate_ref, down_ref, to_ref, fromt_ref,
           out_ref, dx_ref, dup_ref, dgate_ref, ddown_ref,
           xfull, gfull, nfull, gain_rx, gain_cols, up_t, down_t, gate_t,
           up_mat, dgrid_mat, z_mat, dh_mat, ybuf, dmbuf, dgbuf, dm_zero, act_buf, dpre_buf, mbuf, dhbuf, dpg_buf,
           stat_buf, part, rs1, rs2_src, rs2, back_src, back_rx, wgrad, wgrad_rx, wsum, wfull,
           ag_ss, ag_rs, gain_ss, gain_rs, rs1_ss, rs1_rs, rs2_ss, rs2_rs, back_ss, back_rs, w1_ss, w1_rs, w2_ss, w2_rs):
    coefs, chan_loc, _ = x_ref.shape
    degrees = gain_ref.shape[0]
    channels = chan_loc * 4
    vec_count = channels * (coefs - 1)
    hidden = gate_ref.shape[1]
    chunks = dims['chunks']
    blk_count = up_mat.shape[0]
    blk_rows = up_mat.shape[2]
    steps = hidden // SUB // 2
    quarter = wgrad.shape[0] // 4
    me = lax.axis_index('tp')
    my_dp = lax.axis_index('dp')
    sources = (g_ref, x_ref)
    fulls = (gfull, xfull)
    grad, feat = 0, 1
    dxs, outs = 0, 1
    copies = {}

    def send(key, src, dst, ssem, rsem, axis, peer):
        copy = pltpu.make_async_remote_copy(src_ref=src, dst_ref=dst, send_sem=ssem, recv_sem=rsem, device_id={axis: peer}, device_id_type=MESH)
        copy.start()
        copies[key] = copy

    def lanes_of(chunk):
        return pl.ds(chunk * LANES, LANES)

    barrier = pltpu.get_barrier_semaphore()
    for hop in (1, 2, 3):
        pl.semaphore_signal(barrier, inc=1, device_id={'tp': tp_peer(hop)}, device_id_type=MESH)
        pl.semaphore_signal(barrier, inc=1, device_id={'dp': dp_peer(hop)}, device_id_type=MESH)
    pl.semaphore_wait(barrier, 6)

    for hop in (1, 2, 3):
        send(('gain', hop), gain_ref, gain_rx.at[hop - 1], gain_ss.at[hop - 1], gain_rs.at[hop - 1], 'tp', tp_peer(hop))
    for chunk in range(chunks):
        for arr in (grad, feat):
            for hop in (2, 1):
                send(('ag', arr, chunk, hop), sources[arr].at[:, :, lanes_of(chunk)], fulls[arr].at[chunk, :, chan_rows(me, chan_loc), :],
                     ag_ss.at[arr, chunk, hop - 1], ag_rs.at[arr, chunk, hop - 1], 'tp', tp_peer(hop))

    def relay(arr, chunk):
        copies[('ag', arr, chunk, 2)].wait_recv()
        block = fulls[arr].at[chunk, :, chan_rows(tp_peer(2), chan_loc), :]
        send(('ag', arr, chunk, 3), block, block, ag_ss.at[arr, chunk, 2], ag_rs.at[arr, chunk, 2], 'tp', tp_peer(1))

    def gathered(arr, chunk):
        copies[('ag', arr, chunk, 1)].wait_recv()
        copies[('ag', arr, chunk, 3)].wait_recv()

    for chunk in range(chunks):
        for arr in (grad, feat):
            fulls[arr][chunk, :, chan_rows(me, chan_loc), :] = sources[arr][:, :, chunk * LANES:(chunk + 1) * LANES]
    build_grid_mats(to_ref, fromt_ref, up_mat, dgrid_mat, z_mat, dh_mat, dims['blk_pts'])
    for degree in range(degrees):
        up_t[degree] = up_ref[degree].astype(F32).T.astype(BF16)
        down_t[degree] = down_ref[degree].astype(F32).T.astype(BF16)
    gate_t[...] = gate_ref[...].astype(F32).T.astype(BF16)
    for buf in (ybuf, dmbuf):
        tail = 192
        buf[:, tail:, :] = jnp.zeros((buf.shape[0], KPAD - tail, LANES), BF16)
    wgrad[...] = jnp.zeros_like(wgrad)
    back_src[...] = jnp.zeros_like(back_src)

    def gain_block(tp, rows):
        eye = iota2((chan_loc, chan_loc), 0) == iota2((chan_loc, chan_loc), 1)
        for degree in range(degrees):
            col = jnp.sum(jnp.where(eye, rows[degree:degree + 1, :], 0.0), axis=1, keepdims=True)
            gain_cols[degree, chan_rows(tp, chan_loc), :] = jnp.broadcast_to(col, (chan_loc, LANES))

    gain_block(me, gain_ref[...])

    def grad_part(chunk):
        d_mixed = split_coefs([mm(down_ref[degree], lane_cat(gfull, chunk, degree)) for degree in range(degrees)])
        dm_zero[...] = rounded(d_mixed[0])
        for pair in range((coefs - 1) // 2):
            dmbuf[:, 16 * pair:16 * pair + 16, :] = pair_rows(d_mixed[2 * pair + 1], d_mixed[2 * pair + 2])

        def step(idx, carry):
            rhs = step_rhs(dmbuf, idx)
            for blk in range(blk_count):
                store_wide(dgbuf, (idx, blk), mm(load_wide(dgrid_mat, (blk,)), rhs).astype(BF16))
            return carry

        lax.fori_loop(0, steps, step, 0)

    def normalize(chunk):
        scalar = xfull[chunk, 0].astype(F32)
        mean = jnp.sum(scalar, axis=0, keepdims=True) / channels
        centered = scalar - mean
        inv_s = lax.rsqrt(jnp.sum(centered * centered, axis=0, keepdims=True) / channels + NORM_EPS)
        squares = jnp.zeros((channels, LANES), F32)
        for coef in range(1, coefs):
            vec = xfull[chunk, coef].astype(F32)
            squares = squares + vec * vec
        inv_v = lax.rsqrt(jnp.sum(squares, axis=0, keepdims=True) / vec_count + NORM_EPS)
        stat_buf[chunk, 0:1, :] = mean
        stat_buf[chunk, 1:2, :] = inv_s
        stat_buf[chunk, 2:3, :] = inv_v
        nfull[chunk, 0] = (centered * inv_s * gain_cols[0]).astype(BF16)
        for degree in range(1, degrees):
            for coef in degree_span(degree):
                nfull[chunk, coef] = (xfull[chunk, coef].astype(F32) * inv_v * gain_cols[degree]).astype(BF16)

    def hidden_part(chunk):
        hid = split_coefs([mm(up_t[degree], lane_cat(nfull, chunk, degree)) for degree in range(degrees)])
        hid.append(jnp.zeros_like(hid[0]))
        for pair in range((coefs + 1) // 2):
            ybuf[:, 16 * pair:16 * pair + 16, :] = pair_rows(hid[2 * pair], hid[2 * pair + 1])
        half = rounded(mm(gate_t[...], nfull[chunk, 0])) * 0.5
        tan = jnp.tanh(half)
        wide = 1.0 + tan
        act = half * wide
        mbuf[chunk, 0] = act.astype(BF16)
        dpg_buf[chunk] = (dm_zero[...] * (0.5 * (wide + act * (1.0 - tan)))).astype(BF16)

    def grid_front(idx, blk):
        half = rounded(mm(load_wide(up_mat, (blk,)), step_rhs(ybuf, idx)))
        tan = jnp.tanh(half)
        wide = 1.0 + tan
        act = half * wide
        d_pre = load_wide(dgbuf, (idx, blk)).astype(F32) * (wide + act * (1.0 - tan))
        store_wide(act_buf, (blk,), act.astype(BF16))
        store_wide(dpre_buf, (blk,), d_pre.astype(BF16))

    def step_rhs(ref, idx):
        return jnp.concatenate([ref[2 * idx], ref[2 * idx + 1]], axis=1)

    def grid_back(blk):
        pad = jnp.zeros((KPAD - blk_rows, 2 * LANES), BF16)
        z_add = mm(load_wide(z_mat, (blk,)), jnp.concatenate([load_wide(act_buf, (blk,)), pad], axis=0))
        h_add = mm(load_wide(dh_mat, (blk,)), jnp.concatenate([load_wide(dpre_buf, (blk,)), pad], axis=0))
        return z_add, h_add

    def grid_store(chunk, idx, sums):
        rows = pl.ds(pl.multiple_of(16 * idx, 16), 16)

        def by_coef(value, count):
            value = value[:count * SUB].reshape(count, SUB, 2 * LANES)
            return jnp.concatenate([value[:, :, :LANES], value[:, :, LANES:]], axis=1).astype(BF16)

        mbuf[chunk, 1:coefs, rows, :] = by_coef(sums[0], coefs - 1)
        dhbuf[chunk, :, rows, :] = by_coef(sums[1], coefs)

    def grid_both(chunk, idx, front, back):
        sums = None
        for blk in range(blk_count):
            if back:
                adds = grid_back(blk)
                sums = adds if sums is None else (sums[0] + adds[0], sums[1] + adds[1])
            if front:
                grid_front(idx, blk)
        if back:
            grid_store(chunk, idx - 1, sums)

    def grid_part(chunk, first, last):
        def step(idx, carry):
            grid_both(chunk, idx, True, True)
            return carry

        if first == 0:
            grid_both(chunk, 0, True, False)
        lax.fori_loop(max(first, 1), last, step, 0)
        if last == steps:
            grid_both(chunk, steps, False, True)

    def weight_grads(chunk):
        for degree in range(degrees):
            rows = pl.ds(degree * channels, channels)
            wgrad[rows, :] += mm_nt(lane_cat(nfull, chunk, degree), lane_cat(dhbuf, chunk, degree))
            rows = pl.ds((degrees + 1) * channels + degree * hidden, hidden)
            wgrad[rows, :] += mm_nt(lane_cat(mbuf, chunk, degree), lane_cat(gfull, chunk, degree))
        rows = pl.ds(degrees * channels, channels)
        wgrad[rows, :] += mm_nt(nfull[chunk, 0], dpg_buf[chunk])

    def store_part(arr, chunk, per_degree):
        for coef, value in enumerate(split_coefs(per_degree)):
            part[arr, chunk, coef] = value.astype(BF16)

    def input_grads(chunk):
        per_degree = [mm(up_ref[degree], lane_cat(dhbuf, chunk, degree)) for degree in range(degrees)]
        per_degree[0] = per_degree[0] + mm(gate_ref[...], dpg_buf[chunk])
        store_part(dxs, chunk, per_degree)

    def outputs(chunk):
        store_part(outs, chunk, [mm(down_t[degree], lane_cat(mbuf, chunk, degree)) for degree in range(degrees)])

    def scatter_core(arr, chunk):
        for chip in (0, 1):
            rows = chan_rows(2 * chip + 1 - me % 2, chan_loc)
            send(('rs1', arr, chunk, chip), part.at[arr, chunk, :, rows, :], rs1.at[arr, chunk, chip],
                 rs1_ss.at[arr, chunk, chip], rs1_rs.at[arr, chunk, chip], 'tp', tp_peer(1))

    def chip_sum(arr, chunk, chip):
        own = part[arr, chunk, :, chan_rows(2 * chip + me % 2, chan_loc), :].astype(F32)
        return own + rs1[arr, chunk, chip].astype(F32)

    def scatter_chip(arr, chunk):
        for chip in (0, 1):
            copies[('rs1', arr, chunk, chip)].wait_recv()
        rs2_src[arr, chunk] = chip_sum(arr, chunk, 1 - me // 2).astype(BF16)
        send(('rs2', arr, chunk), rs2_src.at[arr, chunk], rs2.at[arr, chunk], rs2_ss.at[arr, chunk], rs2_rs.at[arr, chunk], 'tp', tp_peer(2))

    def scattered(arr, chunk):
        copies[('rs2', arr, chunk)].wait_recv()
        return chip_sum(arr, chunk, me // 2) + rs2[arr, chunk].astype(F32)

    def own_x(chunk):
        return x_ref[:, :, chunk * LANES:(chunk + 1) * LANES].astype(F32)

    def finish_out(chunk):
        out_ref[:, :, chunk * LANES:(chunk + 1) * LANES] = (own_x(chunk) + scattered(outs, chunk)).astype(BF16)

    def own_gain(degree):
        return gain_cols[degree, chan_rows(me, chan_loc), :]

    def back_stats(chunk):
        x_own = own_x(chunk)
        d_norm = rounded(scattered(dxs, chunk))
        rs2[dxs, chunk] = d_norm.astype(BF16)
        d_hat = d_norm[0] * own_gain(0)
        hat = (x_own[0] - stat_buf[chunk, 0:1, :]) * stat_buf[chunk, 1:2, :]
        back_src[chunk, 0:1, :] = jnp.sum(d_hat, axis=0, keepdims=True)
        back_src[chunk, 1:2, :] = jnp.sum(d_hat * hat, axis=0, keepdims=True)
        total = jnp.zeros((chan_loc, LANES), F32)
        for degree in range(1, degrees):
            for coef in degree_span(degree):
                total = total + d_norm[coef] * own_gain(degree) * x_own[coef]
        back_src[chunk, 2:3, :] = jnp.sum(total, axis=0, keepdims=True)
        for hop in (2, 3, 1):
            send(('back', chunk, hop), back_src.at[chunk], back_rx.at[chunk, hop - 1], back_ss.at[chunk, hop - 1], back_rs.at[chunk, hop - 1], 'tp', tp_peer(hop))

    def finish_dx(chunk):
        for hop in (1, 2, 3):
            copies[('back', chunk, hop)].wait_recv()
        sums = (back_src[chunk] + back_rx[chunk, 0]) + (back_rx[chunk, 1] + back_rx[chunk, 2])
        mean, inv_s, inv_v = (stat_buf[chunk, j:j + 1, :] for j in range(3))
        lanes = slice(chunk * LANES, (chunk + 1) * LANES)
        hat = (x_ref[0, :, lanes].astype(F32) - mean) * inv_s
        d_hat = rs2[dxs, chunk, 0].astype(F32) * own_gain(0)
        d_scalar = inv_s * (d_hat - sums[0:1] / channels - hat * (sums[1:2] / channels))
        dx_ref[0, :, lanes] = (d_scalar + g_ref[0, :, lanes].astype(F32)).astype(BF16)
        scale = (inv_v * inv_v * inv_v) * (sums[2:3] / vec_count)
        for degree in range(1, degrees):
            for coef in degree_span(degree):
                d_hat = rs2[dxs, chunk, coef].astype(F32) * own_gain(degree)
                d_vec = inv_v * d_hat - x_ref[coef, :, lanes].astype(F32) * scale
                dx_ref[coef, :, lanes] = (d_vec + g_ref[coef, :, lanes].astype(F32)).astype(BF16)

    def quarter_rows(dp):
        return pl.ds(pl.multiple_of(dp * quarter, 16), quarter)

    def wgrad_scatter():
        for hop in (3, 1, 2):
            send(('w1', hop), wgrad.at[quarter_rows(dp_peer(hop))], wgrad_rx.at[hop - 1], w1_ss.at[hop - 1], w1_rs.at[hop - 1], 'dp', dp_peer(hop))

    def wgrad_reduce():
        for hop in (1, 2, 3):
            copies[('w1', hop)].wait_recv()
        total = (wgrad[quarter_rows(my_dp), :] + wgrad_rx[0]) + (wgrad_rx[1] + wgrad_rx[2])
        wsum[...] = total.astype(BF16)
        wfull[quarter_rows(my_dp), :] = wsum[...]
        for hop in (3, 1, 2):
            send(('w2', hop), wsum, wfull.at[quarter_rows(my_dp)], w2_ss.at[hop - 1], w2_rs.at[hop - 1], 'dp', dp_peer(hop))

    def wgrad_finish():
        for hop in (1, 2, 3):
            copies[('w2', hop)].wait_recv()
        dup_ref[...] = wfull[:degrees * channels, :]
        dgate_ref[...] = wfull[degrees * channels:(degrees + 1) * channels, :]
        ddown_ref[...] = wfull[(degrees + 1) * channels:, :]

    relay(grad, 0)
    for hop in (1, 2, 3):
        copies[('gain', hop)].wait_recv()
        gain_block(tp_peer(hop), gain_rx[hop - 1])
    gathered(grad, 0)
    grad_part(0)
    relay(feat, 0)
    gathered(feat, 0)
    normalize(0)
    hidden_part(0)
    grid_part(0, 0, steps // 2)
    relay(grad, 1)
    grid_part(0, steps // 2, steps)
    weight_grads(0)
    input_grads(0)
    scatter_core(dxs, 0)
    outputs(0)
    scatter_core(outs, 0)
    relay(feat, 1)
    scatter_chip(dxs, 0)
    gathered(grad, 1)
    grad_part(1)
    scatter_chip(outs, 0)
    gathered(feat, 1)
    normalize(1)
    hidden_part(1)
    grid_part(1, 0, steps)
    weight_grads(1)
    wgrad_scatter()
    input_grads(1)
    scatter_core(dxs, 1)
    outputs(1)
    scatter_chip(dxs, 1)
    scatter_core(outs, 1)
    back_stats(0)
    scatter_chip(outs, 1)
    finish_out(0)
    finish_dx(0)
    wgrad_reduce()
    back_stats(1)
    finish_out(1)
    finish_dx(1)
    wgrad_finish()
    for copy in copies.values():
        copy.wait_send()


def solution(mesh):
    act_spec = P('dp', None, 'tp')
    in_specs = (act_spec, P(None, 'tp'), P(None, None, 'tp'), P(None, 'tp'), P(None, 'tp', None), P(None, None), P(None, None), act_spec)
    out_specs = (act_spec, act_spec, P(None, None, 'tp'), P(None, 'tp'), P(None, 'tp', None))

    def local_step(x_loc, gain_loc, up_loc, gate_loc, down_loc, to_grid, from_grid, grad_loc):
        nodes, coefs, chan_loc = x_loc.shape
        degrees, channels, hidden = up_loc.shape
        points = to_grid.shape[1]
        blk_pts = 28
        blks = points // blk_pts
        chunks = nodes // LANES
        groups = hidden // SUB
        w_rows = degrees * channels + channels + degrees * hidden
        dma = pltpu.SemaphoreType.DMA

        def vm(*shape, dtype=BF16):
            return pltpu.VMEM(shape, dtype)

        full = (chunks, coefs, channels, LANES)
        scratch = [
            vm(*full), vm(*full), vm(*full),
            vm(3, degrees, chan_loc, dtype=F32), vm(degrees, channels, LANES, dtype=F32),
            vm(degrees, hidden, channels), vm(degrees, channels, hidden), vm(hidden, channels),
            vm(blks, 2, blk_pts * SUB, LANES), vm(blks, 2, blk_pts * SUB, LANES), vm(blks, 2, (coefs - 1) * SUB, LANES), vm(blks, 2, (coefs + 1) * SUB, LANES),
            vm(groups, KPAD, LANES), vm(groups, KPAD, LANES), vm(groups // 2, blks, 2, blk_pts * SUB, LANES),
            vm(hidden, LANES, dtype=F32), vm(blks, 2, blk_pts * SUB, LANES), vm(blks, 2, blk_pts * SUB, LANES), vm(chunks, coefs, hidden, LANES), vm(chunks, coefs, hidden, LANES), vm(chunks, hidden, LANES),
            vm(chunks, SUB, LANES, dtype=F32),
            vm(2, *full), vm(2, chunks, 2, coefs, chan_loc, LANES), vm(2, chunks, coefs, chan_loc, LANES), vm(2, chunks, coefs, chan_loc, LANES),
            vm(chunks, SUB, LANES, dtype=F32), vm(chunks, 3, SUB, LANES, dtype=F32),
            vm(w_rows, hidden, dtype=F32), vm(3, w_rows // 4, hidden, dtype=F32), vm(w_rows // 4, hidden), vm(w_rows, hidden),
            dma((2, chunks, 3)), dma((2, chunks, 3)), dma((3,)), dma((3,)),
            dma((2, chunks, 2)), dma((2, chunks, 2)), dma((2, chunks)), dma((2, chunks)),
            dma((chunks, 3)), dma((chunks, 3)), dma((3,)), dma((3,)), dma((3,)), dma((3,)),
        ]
        vmem = pl.BlockSpec(memory_space=pltpu.VMEM)
        act = jax.ShapeDtypeStruct((coefs, chan_loc, nodes), BF16)
        out_t, dx_t, d_up, d_gate, d_down = pl.pallas_call(
            functools.partial(kernel, {'chunks': chunks, 'blk_pts': blk_pts}),
            out_shape=(act, act, jax.ShapeDtypeStruct((degrees * channels, hidden), BF16), jax.ShapeDtypeStruct((channels, hidden), BF16), jax.ShapeDtypeStruct((degrees * hidden, channels), BF16)),
            in_specs=[vmem] * 8,
            out_specs=(vmem,) * 5,
            scratch_shapes=scratch,
            compiler_params=pltpu.CompilerParams(collective_id=0, has_side_effects=True, vmem_limit_bytes=60 * 1024 * 1024),
            name='s2_ffn',
        )(x_loc.transpose(1, 2, 0), grad_loc.transpose(1, 2, 0), gain_loc, up_loc, gate_loc, down_loc, to_grid, from_grid.T)
        return (out_t.transpose(2, 0, 1), dx_t.transpose(2, 0, 1), d_up.reshape(degrees, channels, hidden), d_gate, d_down.reshape(degrees, hidden, channels))

    return jax.shard_map(local_step, mesh=mesh, in_specs=in_specs, out_specs=out_specs, check_vma=False)
```

```python
import functools
import math
import jax
import jax.numpy as jnp
from jax import lax
from jax.experimental import pallas as pl
from jax.experimental.pallas import tpu as pltpu
from jax.sharding import PartitionSpec as P

NORM_EPS = 1e-5
F32 = jnp.float32
BF16 = jnp.bfloat16
MESH = pl.DeviceIdType.MESH
LANES = 128
SUB = 8
KPAD = 256


def mm(lhs, rhs):
    return jnp.dot(lhs, rhs, preferred_element_type=F32)


def mm_nt(lhs, rhs):
    return lax.dot_general(lhs, rhs, (((1,), (1,)), ((), ())), preferred_element_type=F32)


def degree_span(degree):
    return range(degree * degree, (degree + 1) * (degree + 1))


def lane_cat(ref, chunk, degree):
    parts = [ref[chunk, coef] for coef in degree_span(degree)]
    return parts[0] if len(parts) == 1 else jnp.concatenate(parts, axis=1)


def pair_rows(first, second):
    groups = first.shape[0] // SUB
    shape = (groups, SUB, first.shape[1])
    return jnp.concatenate([first.reshape(shape), second.reshape(shape)], axis=1).astype(BF16)


def split_coefs(per_degree):
    out = []
    for degree, value in enumerate(per_degree):
        out += [value[:, LANES * j:LANES * (j + 1)] for j in range(2 * degree + 1)]
    return out


def rounded(value):
    return value.astype(BF16).astype(F32)


def iota2(shape, axis):
    return lax.broadcasted_iota(jnp.int32, shape, axis)


def ones_where(cond):
    return jnp.where(cond, 1.0, 0.0).astype(BF16)


def dp_peer(hop):
    dp = lax.axis_index('dp')
    zpos, ypos = dp // 2, dp % 2
    if hop % 2:
        ypos = 1 - ypos
    if hop // 2:
        zpos = 1 - zpos
    return zpos * 2 + ypos


def tp_peer(hop):
    tp = lax.axis_index('tp')
    xpos, core = tp // 2, tp % 2
    if hop % 2:
        core = 1 - core
    if hop // 2:
        xpos = 1 - xpos
    return xpos * 2 + core


def chan_rows(tp, chan_loc):
    return pl.ds(pl.multiple_of(tp * chan_loc, chan_loc), chan_loc)


def load_wide(ref, index):
    return jnp.concatenate([ref[index + (0,)], ref[index + (1,)]], axis=1)


def store_wide(ref, index, value):
    ref[index + (0,)] = value[:, :LANES]
    ref[index + (1,)] = value[:, LANES:]


def build_grid_mats(to_ref, fromt_ref, up_mat, dgrid_mat, z_mat, dh_mat, blk_pts):
    coefs, points = to_ref.shape
    vecs = fromt_ref.shape[0]
    blk_rows = blk_pts * SUB
    to_b = to_ref[...].astype(BF16)
    from_b = fromt_ref[...].astype(BF16)

    def spread(count, shape, axis):
        return ones_where(iota2(shape, axis) // SUB == iota2(shape, 1 - axis))

    to_cols = lax.dot_general(to_b, spread(coefs, (coefs, KPAD), 1), (((0,), (0,)), ((), ())), preferred_element_type=F32)
    from_cols = lax.dot_general(from_b, spread(vecs, (vecs, KPAD), 1), (((0,), (0,)), ((), ())), preferred_element_type=F32)
    to_cols = (to_cols * 0.5).astype(BF16)
    from_cols = (from_cols * 0.5).astype(BF16)
    to_rows = mm(spread(coefs, (dh_mat.shape[2], coefs), 0), to_b).astype(BF16)
    from_rows = mm(spread(vecs, (z_mat.shape[2], vecs), 0), from_b).astype(BF16)

    def diagonal(value):
        same = iota2(value.shape, 0) % SUB == iota2(value.shape, 1) % SUB
        return jnp.where(same, value, 0.0).astype(BF16)

    def blk_step(blk, carry):
        first = blk * blk_pts
        shape = (blk_rows, points)
        pick = ones_where(iota2(shape, 0) // SUB + first == iota2(shape, 1))
        shape = (points, KPAD)
        col = iota2(shape, 1)
        pick_t = ones_where((col // SUB + first == iota2(shape, 0)) & (col < blk_rows))
        store_wide(up_mat, (blk,), diagonal(mm(pick, to_cols)))
        store_wide(dgrid_mat, (blk,), diagonal(mm(pick, from_cols)))
        store_wide(z_mat, (blk,), diagonal(mm(from_rows, pick_t)))
        store_wide(dh_mat, (blk,), diagonal(mm(to_rows, pick_t)))
        return carry

    lax.fori_loop(0, points // blk_pts, blk_step, 0)


def kernel(dims, x_ref, g_ref, gain_ref, up_ref, gate_ref, down_ref, to_ref, fromt_ref,
           out_ref, dx_ref, dup_ref, dgate_ref, ddown_ref,
           xfull, gfull, nfull, gain_rx, gain_cols, up_t, down_t, gate_t,
           up_mat, dgrid_mat, z_mat, dh_mat, ybuf, dmbuf, slope_buf, gate_slope, half_buf, act_buf, dpre_buf, mbuf, dhbuf, dpg_buf,
           stat_buf, part, rs1, rs2_src, rs2, back_src, back_rx, wdown_acc, wup_acc, wdown_rx, wup_rx, wdown_sum, wup_sum, wdown_full, wup_full,
           ag_ss, ag_rs, gain_ss, gain_rs, rs1_ss, rs1_rs, rs2_ss, rs2_rs, back_ss, back_rs, w1_ss, w1_rs, w2_ss, w2_rs):
    coefs, chan_loc, _ = x_ref.shape
    degrees = gain_ref.shape[0]
    channels = chan_loc * 4
    vec_count = channels * (coefs - 1)
    hidden = gate_ref.shape[1]
    chunks = dims['chunks']
    blk_count = up_mat.shape[0]
    blk_rows = up_mat.shape[2]
    steps = hidden // SUB // 2
    wgrad = (wdown_acc, wup_acc)
    wgrad_rx = (wdown_rx, wup_rx)
    wsum = (wdown_sum, wup_sum)
    wfull = (wdown_full, wup_full)
    me = lax.axis_index('tp')
    my_dp = lax.axis_index('dp')
    sources = (g_ref, x_ref)
    fulls = (gfull, xfull)
    grad, feat = 0, 1
    dxs, outs = 0, 1
    copies = {}

    def send(key, src, dst, ssem, rsem, axis, peer):
        copy = pltpu.make_async_remote_copy(src_ref=src, dst_ref=dst, send_sem=ssem, recv_sem=rsem, device_id={axis: peer}, device_id_type=MESH)
        copy.start()
        copies[key] = copy

    def lanes_of(chunk):
        return pl.ds(chunk * LANES, LANES)

    barrier = pltpu.get_barrier_semaphore()
    for hop in (1, 2, 3):
        pl.semaphore_signal(barrier, inc=1, device_id={'tp': tp_peer(hop)}, device_id_type=MESH)
        pl.semaphore_signal(barrier, inc=1, device_id={'dp': dp_peer(hop)}, device_id_type=MESH)
    pl.semaphore_wait(barrier, 6)

    for hop in (1, 2, 3):
        send(('gain', hop), gain_ref, gain_rx.at[hop - 1], gain_ss.at[hop - 1], gain_rs.at[hop - 1], 'tp', tp_peer(hop))
    for chunk in range(chunks):
        for arr in (feat, grad):
            for hop in (2, 1):
                send(('ag', arr, chunk, hop), sources[arr].at[:, :, lanes_of(chunk)], fulls[arr].at[chunk, :, chan_rows(me, chan_loc), :],
                     ag_ss.at[arr, chunk, hop - 1], ag_rs.at[arr, chunk, hop - 1], 'tp', tp_peer(hop))

    def relay(arr, chunk):
        copies[('ag', arr, chunk, 2)].wait_recv()
        block = fulls[arr].at[chunk, :, chan_rows(tp_peer(2), chan_loc), :]
        send(('ag', arr, chunk, 3), block, block, ag_ss.at[arr, chunk, 2], ag_rs.at[arr, chunk, 2], 'tp', tp_peer(1))

    def gathered(arr, chunk):
        copies[('ag', arr, chunk, 1)].wait_recv()
        copies[('ag', arr, chunk, 3)].wait_recv()

    for chunk in range(chunks):
        for arr in (grad, feat):
            fulls[arr][chunk, :, chan_rows(me, chan_loc), :] = sources[arr][:, :, chunk * LANES:(chunk + 1) * LANES]
    build_grid_mats(to_ref, fromt_ref, up_mat, dgrid_mat, z_mat, dh_mat, dims['blk_pts'])
    for degree in range(degrees):
        up_t[degree] = up_ref[degree].astype(F32).T.astype(BF16)
        down_t[degree] = down_ref[degree].astype(F32).T.astype(BF16)
    gate_t[...] = gate_ref[...].astype(F32).T.astype(BF16)
    for buf in (ybuf, dmbuf):
        tail = 192
        buf[:, tail:, :] = jnp.zeros((buf.shape[0], KPAD - tail, LANES), BF16)
    for acc in wgrad:
        acc[...] = jnp.zeros_like(acc)
    back_src[...] = jnp.zeros_like(back_src)

    def gain_block(tp, rows):
        eye = iota2((chan_loc, chan_loc), 0) == iota2((chan_loc, chan_loc), 1)
        for degree in range(degrees):
            col = jnp.sum(jnp.where(eye, rows[degree:degree + 1, :], 0.0), axis=1, keepdims=True)
            gain_cols[degree, chan_rows(tp, chan_loc), :] = jnp.broadcast_to(col, (chan_loc, LANES))

    gain_block(me, gain_ref[...])

    def normalize(chunk):
        scalar = xfull[chunk, 0].astype(F32)
        mean = jnp.sum(scalar, axis=0, keepdims=True) / channels
        centered = scalar - mean
        inv_s = lax.rsqrt(jnp.sum(centered * centered, axis=0, keepdims=True) / channels + NORM_EPS)
        squares = jnp.zeros((channels, LANES), F32)
        for coef in range(1, coefs):
            vec = xfull[chunk, coef].astype(F32)
            squares = squares + vec * vec
        inv_v = lax.rsqrt(jnp.sum(squares, axis=0, keepdims=True) / vec_count + NORM_EPS)
        stat_buf[chunk, 0:1, :] = mean
        stat_buf[chunk, 1:2, :] = inv_s
        stat_buf[chunk, 2:3, :] = inv_v
        nfull[chunk, 0] = (centered * inv_s * gain_cols[0]).astype(BF16)
        for degree in range(1, degrees):
            for coef in degree_span(degree):
                nfull[chunk, coef] = (xfull[chunk, coef].astype(F32) * inv_v * gain_cols[degree]).astype(BF16)

    def step_rhs(ref, idx):
        return jnp.concatenate([ref[2 * idx], ref[2 * idx + 1]], axis=1)

    def silu_pair(half):
        tan = jnp.tanh(half)
        wide = 1.0 + tan
        act = half * wide
        return act, wide + act * (1.0 - tan)

    def hidden_part(chunk):
        hid = split_coefs([mm(up_t[degree], lane_cat(nfull, chunk, degree)) for degree in range(degrees)])
        hid.append(jnp.zeros_like(hid[0]))
        for pair in range((coefs + 1) // 2):
            ybuf[:, 16 * pair:16 * pair + 16, :] = pair_rows(hid[2 * pair], hid[2 * pair + 1])
        act, slope = silu_pair(rounded(mm(gate_t[...], nfull[chunk, 0])) * 0.5)
        mbuf[chunk, 0] = act.astype(BF16)
        gate_slope[...] = 0.5 * slope

    def grad_part(chunk):
        d_mixed = split_coefs([mm(down_ref[degree], lane_cat(gfull, chunk, degree)) for degree in range(degrees)])
        dpg_buf[chunk] = (rounded(d_mixed[0]) * gate_slope[...]).astype(BF16)
        for pair in range((coefs - 1) // 2):
            dmbuf[:, 16 * pair:16 * pair + 16, :] = pair_rows(d_mixed[2 * pair + 1], d_mixed[2 * pair + 2])

    def to_points(idx, blk):
        store_wide(half_buf, (blk,), mm(load_wide(up_mat, (blk,)), step_rhs(ybuf, idx)).astype(BF16))

    def on_points(idx, blk):
        act, slope = silu_pair(load_wide(half_buf, (blk,)).astype(F32))
        store_wide(act_buf, (blk,), act.astype(BF16))
        store_wide(slope_buf, (idx, blk), slope)

    def grad_points(idx, blk):
        d_half = rounded(mm(load_wide(dgrid_mat, (blk,)), step_rhs(dmbuf, idx)))
        store_wide(dpre_buf, (blk,), (d_half * load_wide(slope_buf, (idx, blk))).astype(BF16))

    def from_points(mat, buf, blk):
        pad = jnp.zeros((KPAD - blk_rows, 2 * LANES), BF16)
        return mm(load_wide(mat, (blk,)), jnp.concatenate([load_wide(buf, (blk,)), pad], axis=0))

    def store_coefs(dst, chunk, first, idx, value):
        count = coefs - first
        value = value[:count * SUB].reshape(count, SUB, 2 * LANES)
        rows = pl.ds(pl.multiple_of(16 * idx, 16), 16)
        dst[chunk, first:coefs, rows, :] = jnp.concatenate([value[:, :, :LANES], value[:, :, LANES:]], axis=1).astype(BF16)

    def forward_turn(chunk, idx, front, mid, back):
        total = None
        for blk in range(blk_count):
            if back:
                add = from_points(z_mat, act_buf, blk)
                total = add if total is None else total + add
            if mid:
                on_points(idx - 1, blk)
            if front:
                to_points(idx, blk)
        if back:
            store_coefs(mbuf, chunk, 1, idx - 2, total)

    def backward_turn(chunk, idx, front, back):
        total = None
        for blk in range(blk_count):
            if back:
                add = from_points(dh_mat, dpre_buf, blk)
                total = add if total is None else total + add
            if front:
                grad_points(idx, blk)
        if back:
            store_coefs(dhbuf, chunk, 0, idx - 1, total)

    def loop(turn, first, last):
        def body(idx, carry):
            turn(idx)
            return carry

        lax.fori_loop(first, last, body, 0)

    def forward_grid(chunk, between):
        full = functools.partial(forward_turn, chunk, front=True, mid=True, back=True)
        forward_turn(chunk, 0, True, False, False)
        forward_turn(chunk, 1, True, True, False)
        loop(full, 2, steps // 2 + 1)
        between()
        loop(full, steps // 2 + 1, steps)
        forward_turn(chunk, steps, False, True, True)
        forward_turn(chunk, steps + 1, False, False, True)

    def backward_grid(chunk, between):
        full = functools.partial(backward_turn, chunk, front=True, back=True)
        backward_turn(chunk, 0, True, False)
        loop(full, 1, steps // 2 + 1)
        between()
        loop(full, steps // 2 + 1, steps)
        backward_turn(chunk, steps, False, True)

    def down_grads(chunk):
        for degree in range(degrees):
            rows = pl.ds(degree * hidden, hidden)
            wgrad[0][rows, :] += mm_nt(lane_cat(mbuf, chunk, degree), lane_cat(gfull, chunk, degree))

    def up_grads(chunk):
        for degree in range(degrees):
            rows = pl.ds(degree * channels, channels)
            wgrad[1][rows, :] += mm_nt(lane_cat(nfull, chunk, degree), lane_cat(dhbuf, chunk, degree))
        rows = pl.ds(degrees * channels, channels)
        wgrad[1][rows, :] += mm_nt(nfull[chunk, 0], dpg_buf[chunk])

    def store_part(arr, chunk, per_degree):
        for coef, value in enumerate(split_coefs(per_degree)):
            part[arr, chunk, coef] = value.astype(BF16)

    def input_grads(chunk):
        per_degree = [mm(up_ref[degree], lane_cat(dhbuf, chunk, degree)) for degree in range(degrees)]
        per_degree[0] = per_degree[0] + mm(gate_ref[...], dpg_buf[chunk])
        store_part(dxs, chunk, per_degree)

    def outputs(chunk):
        store_part(outs, chunk, [mm(down_t[degree], lane_cat(mbuf, chunk, degree)) for degree in range(degrees)])

    def scatter_core(arr, chunk):
        for chip in (0, 1):
            rows = chan_rows(2 * chip + 1 - me % 2, chan_loc)
            send(('rs1', arr, chunk, chip), part.at[arr, chunk, :, rows, :], rs1.at[arr, chunk, chip],
                 rs1_ss.at[arr, chunk, chip], rs1_rs.at[arr, chunk, chip], 'tp', tp_peer(1))

    def chip_sum(arr, chunk, chip):
        own = part[arr, chunk, :, chan_rows(2 * chip + me % 2, chan_loc), :].astype(F32)
        return own + rs1[arr, chunk, chip].astype(F32)

    def scatter_chip(arr, chunk):
        for chip in (0, 1):
            copies[('rs1', arr, chunk, chip)].wait_recv()
        rs2_src[arr, chunk] = chip_sum(arr, chunk, 1 - me // 2).astype(BF16)
        send(('rs2', arr, chunk), rs2_src.at[arr, chunk], rs2.at[arr, chunk], rs2_ss.at[arr, chunk], rs2_rs.at[arr, chunk], 'tp', tp_peer(2))

    def scattered(arr, chunk):
        copies[('rs2', arr, chunk)].wait_recv()
        return chip_sum(arr, chunk, me // 2) + rs2[arr, chunk].astype(F32)

    def own_x(chunk):
        return x_ref[:, :, chunk * LANES:(chunk + 1) * LANES].astype(F32)

    def finish_out(chunk):
        out_ref[:, :, chunk * LANES:(chunk + 1) * LANES] = (own_x(chunk) + scattered(outs, chunk)).astype(BF16)

    def own_gain(degree):
        return gain_cols[degree, chan_rows(me, chan_loc), :]

    def back_stats(chunk):
        x_own = own_x(chunk)
        d_norm = rounded(scattered(dxs, chunk))
        rs2[dxs, chunk] = d_norm.astype(BF16)
        d_hat = d_norm[0] * own_gain(0)
        hat = (x_own[0] - stat_buf[chunk, 0:1, :]) * stat_buf[chunk, 1:2, :]
        back_src[chunk, 0:1, :] = jnp.sum(d_hat, axis=0, keepdims=True)
        back_src[chunk, 1:2, :] = jnp.sum(d_hat * hat, axis=0, keepdims=True)
        total = jnp.zeros((chan_loc, LANES), F32)
        for degree in range(1, degrees):
            for coef in degree_span(degree):
                total = total + d_norm[coef] * own_gain(degree) * x_own[coef]
        back_src[chunk, 2:3, :] = jnp.sum(total, axis=0, keepdims=True)
        for hop in (2, 3, 1):
            send(('back', chunk, hop), back_src.at[chunk], back_rx.at[chunk, hop - 1], back_ss.at[chunk, hop - 1], back_rs.at[chunk, hop - 1], 'tp', tp_peer(hop))

    def finish_dx(chunk):
        for hop in (1, 2, 3):
            copies[('back', chunk, hop)].wait_recv()
        sums = (back_src[chunk] + back_rx[chunk, 0]) + (back_rx[chunk, 1] + back_rx[chunk, 2])
        mean, inv_s, inv_v = (stat_buf[chunk, j:j + 1, :] for j in range(3))
        lanes = slice(chunk * LANES, (chunk + 1) * LANES)
        hat = (x_ref[0, :, lanes].astype(F32) - mean) * inv_s
        d_hat = rs2[dxs, chunk, 0].astype(F32) * own_gain(0)
        d_scalar = inv_s * (d_hat - sums[0:1] / channels - hat * (sums[1:2] / channels))
        dx_ref[0, :, lanes] = (d_scalar + g_ref[0, :, lanes].astype(F32)).astype(BF16)
        scale = (inv_v * inv_v * inv_v) * (sums[2:3] / vec_count)
        for degree in range(1, degrees):
            for coef in degree_span(degree):
                d_hat = rs2[dxs, chunk, coef].astype(F32) * own_gain(degree)
                d_vec = inv_v * d_hat - x_ref[coef, :, lanes].astype(F32) * scale
                dx_ref[coef, :, lanes] = (d_vec + g_ref[coef, :, lanes].astype(F32)).astype(BF16)

    def quarter_rows(group, dp):
        quarter = wgrad[group].shape[0] // 4
        return pl.ds(pl.multiple_of(dp * quarter, 16), quarter)

    def wgrad_scatter(group):
        for hop in (3, 1, 2):
            send(('w1', group, hop), wgrad[group].at[quarter_rows(group, dp_peer(hop))], wgrad_rx[group].at[hop - 1],
                 w1_ss.at[group, hop - 1], w1_rs.at[group, hop - 1], 'dp', dp_peer(hop))

    def wgrad_reduce(group):
        for hop in (1, 2, 3):
            copies[('w1', group, hop)].wait_recv()
        mine = quarter_rows(group, my_dp)
        got = wgrad_rx[group]
        total = ((wgrad[group][mine, :] + got[0]) + (got[1] + got[2])).astype(BF16)
        wsum[group][...] = total
        wfull[group][mine, :] = total
        for hop in (3, 1, 2):
            send(('w2', group, hop), wsum[group], wfull[group].at[mine], w2_ss.at[group, hop - 1], w2_rs.at[group, hop - 1], 'dp', dp_peer(hop))

    def wgrad_finish(group):
        for hop in (1, 2, 3):
            copies[('w2', group, hop)].wait_recv()
        if group == 0:
            ddown_ref[...] = wfull[0][...]
        else:
            dup_ref[...] = wfull[1][:degrees * channels, :]
            dgate_ref[...] = wfull[1][degrees * channels:, :]

    relay(feat, 0)
    for hop in (1, 2, 3):
        copies[('gain', hop)].wait_recv()
        gain_block(tp_peer(hop), gain_rx[hop - 1])
    gathered(feat, 0)
    normalize(0)
    hidden_part(0)
    forward_grid(0, lambda: relay(grad, 0))
    outputs(0)
    scatter_core(outs, 0)
    gathered(grad, 0)
    grad_part(0)
    scatter_chip(outs, 0)
    backward_grid(0, lambda: relay(feat, 1))
    input_grads(0)
    scatter_core(dxs, 0)
    down_grads(0)
    up_grads(0)
    scatter_chip(dxs, 0)
    gathered(feat, 1)
    normalize(1)
    hidden_part(1)
    forward_grid(1, lambda: relay(grad, 1))
    outputs(1)
    scatter_core(outs, 1)
    gathered(grad, 1)
    grad_part(1)
    down_grads(1)
    wgrad_scatter(0)
    scatter_chip(outs, 1)
    finish_out(0)
    backward_grid(1, lambda: back_stats(0))
    input_grads(1)
    scatter_core(dxs, 1)
    up_grads(1)
    wgrad_scatter(1)
    scatter_chip(dxs, 1)
    wgrad_reduce(0)
    finish_dx(0)
    finish_out(1)
    wgrad_reduce(1)
    back_stats(1)
    wgrad_finish(0)
    finish_dx(1)
    wgrad_finish(1)
    for copy in copies.values():
        copy.wait_send()


def hand_on(*refs):
    count = len(refs) // 2
    for src, dst in zip(refs[:count], refs[count:]):
        dst[...] = src[...]


def solution(mesh):
    act_spec = P('dp', None, 'tp')
    in_specs = (act_spec, P(None, 'tp'), P(None, None, 'tp'), P(None, 'tp'), P(None, 'tp', None), P(None, None), P(None, None), act_spec)
    out_specs = (act_spec, act_spec, P(None, None, 'tp'), P(None, 'tp'), P(None, 'tp', None))

    def local_step(x_loc, gain_loc, up_loc, gate_loc, down_loc, to_grid, from_grid, grad_loc):
        nodes, coefs, chan_loc = x_loc.shape
        degrees, channels, hidden = up_loc.shape
        points = to_grid.shape[1]
        blk_pts = 28
        blks = points // blk_pts
        chunks = nodes // LANES
        groups = hidden // SUB
        down_rows = degrees * hidden
        up_rows = degrees * channels + channels
        dma = pltpu.SemaphoreType.DMA

        def vm(*shape, dtype=BF16):
            return pltpu.VMEM(shape, dtype)

        full = (chunks, coefs, channels, LANES)
        ins = (x_loc.transpose(1, 2, 0), grad_loc.transpose(1, 2, 0), gain_loc, up_loc, gate_loc, down_loc, to_grid, from_grid.T)
        scratch = [
            vm(*full), vm(*full), vm(*full),
            vm(3, degrees, chan_loc, dtype=F32), vm(degrees, channels, LANES, dtype=F32),
            vm(degrees, hidden, channels), vm(degrees, channels, hidden), vm(hidden, channels),
            vm(blks, 2, blk_pts * SUB, LANES), vm(blks, 2, blk_pts * SUB, LANES), vm(blks, 2, (coefs - 1) * SUB, LANES), vm(blks, 2, (coefs + 1) * SUB, LANES),
            vm(groups, KPAD, LANES), vm(groups, KPAD, LANES), vm(groups // 2, blks, 2, blk_pts * SUB, LANES, dtype=F32),
            vm(hidden, LANES, dtype=F32), vm(blks, 2, blk_pts * SUB, LANES), vm(blks, 2, blk_pts * SUB, LANES), vm(blks, 2, blk_pts * SUB, LANES), vm(chunks, coefs, hidden, LANES), vm(chunks, coefs, hidden, LANES), vm(chunks, hidden, LANES),
            vm(chunks, SUB, LANES, dtype=F32),
            vm(2, *full), vm(2, chunks, 2, coefs, chan_loc, LANES), vm(2, chunks, coefs, chan_loc, LANES), vm(2, chunks, coefs, chan_loc, LANES),
            vm(chunks, SUB, LANES, dtype=F32), vm(chunks, 3, SUB, LANES, dtype=F32),
            vm(down_rows, LANES, dtype=F32), vm(up_rows, LANES, dtype=F32), vm(3, down_rows // 4, LANES, dtype=F32), vm(3, up_rows // 4, LANES, dtype=F32),
            vm(down_rows // 4, LANES), vm(up_rows // 4, LANES), vm(down_rows, LANES), vm(up_rows, LANES),
            dma((2, chunks, 3)), dma((2, chunks, 3)), dma((3,)), dma((3,)),
            dma((2, chunks, 2)), dma((2, chunks, 2)), dma((2, chunks)), dma((2, chunks)),
            dma((chunks, 3)), dma((chunks, 3)), dma((2, 3)), dma((2, 3)), dma((2, 3)), dma((2, 3)),
        ]
        vmem = pl.BlockSpec(memory_space=pltpu.VMEM)
        act = jax.ShapeDtypeStruct((coefs, chan_loc, nodes), BF16)
        shapes = (act, act, jax.ShapeDtypeStruct((degrees * channels, hidden), BF16), jax.ShapeDtypeStruct((channels, hidden), BF16), jax.ShapeDtypeStruct((degrees * hidden, channels), BF16))
        results = pl.pallas_call(
            functools.partial(kernel, {'chunks': chunks, 'blk_pts': blk_pts}),
            out_shape=shapes,
            in_specs=[vmem] * len(ins),
            out_specs=(vmem,) * 5,
            scratch_shapes=scratch,
            compiler_params=pltpu.CompilerParams(collective_id=0, has_side_effects=True, vmem_limit_bytes=62 * 1024 * 1024),
            name='s2_ffn',
        )(*ins)
        out_t, dx_t, d_up, d_gate, d_down = pl.pallas_call(
            hand_on,
            out_shape=shapes,
            in_specs=[vmem] * 5,
            out_specs=(vmem,) * 5,
            compiler_params=pltpu.CompilerParams(vmem_limit_bytes=62 * 1024 * 1024),
            name='hand_on',
        )(*results)
        return (out_t.transpose(2, 0, 1), dx_t.transpose(2, 0, 1), d_up.reshape(degrees, channels, hidden), d_gate, d_down.reshape(degrees, hidden, channels))

    return jax.shard_map(local_step, mesh=mesh, in_specs=in_specs, out_specs=out_specs, check_vma=False)
```

```python
import functools
import math
import jax
import jax.numpy as jnp
from jax import lax
from jax.experimental import pallas as pl
from jax.experimental.pallas import tpu as pltpu
from jax.sharding import PartitionSpec as P

NORM_EPS = 1e-5
F32 = jnp.float32
BF16 = jnp.bfloat16
MESH = pl.DeviceIdType.MESH
LANES = 128
SUB = 8
KPAD = 256


def mm(lhs, rhs):
    return jnp.dot(lhs, rhs, preferred_element_type=F32)


def mm_nt(lhs, rhs):
    return lax.dot_general(lhs, rhs, (((1,), (1,)), ((), ())), preferred_element_type=F32)


def degree_span(degree):
    return range(degree * degree, (degree + 1) * (degree + 1))


def lane_cat(ref, chunk, degree):
    parts = [ref[chunk, coef] for coef in degree_span(degree)]
    return parts[0] if len(parts) == 1 else jnp.concatenate(parts, axis=1)


def pair_rows(first, second):
    groups = first.shape[0] // SUB
    shape = (groups, SUB, first.shape[1])
    return jnp.concatenate([first.reshape(shape), second.reshape(shape)], axis=1).astype(BF16)


def split_coefs(per_degree):
    out = []
    for degree, value in enumerate(per_degree):
        out += [value[:, LANES * j:LANES * (j + 1)] for j in range(2 * degree + 1)]
    return out


def rounded(value):
    return value.astype(BF16).astype(F32)


def iota2(shape, axis):
    return lax.broadcasted_iota(jnp.int32, shape, axis)


def ones_where(cond):
    return jnp.where(cond, 1.0, 0.0).astype(BF16)


def dp_peer(hop):
    dp = lax.axis_index('dp')
    zpos, ypos = dp // 2, dp % 2
    if hop % 2:
        ypos = 1 - ypos
    if hop // 2:
        zpos = 1 - zpos
    return zpos * 2 + ypos


def tp_peer(hop):
    tp = lax.axis_index('tp')
    xpos, core = tp // 2, tp % 2
    if hop % 2:
        core = 1 - core
    if hop // 2:
        xpos = 1 - xpos
    return xpos * 2 + core


def chan_rows(tp, chan_loc):
    return pl.ds(pl.multiple_of(tp * chan_loc, chan_loc), chan_loc)


def load_wide(ref, index):
    return jnp.concatenate([ref[index + (0,)], ref[index + (1,)]], axis=1)


def store_wide(ref, index, value):
    ref[index + (0,)] = value[:, :LANES]
    ref[index + (1,)] = value[:, LANES:]


def build_grid_mats(to_ref, fromt_ref, up_mat, dgrid_mat, z_mat, dh_mat, blk_pts):
    coefs, points = to_ref.shape
    vecs = fromt_ref.shape[0]
    blk_rows = blk_pts * SUB
    to_b = to_ref[...].astype(BF16)
    from_b = fromt_ref[...].astype(BF16)

    def spread(count, shape, axis):
        return ones_where(iota2(shape, axis) // SUB == iota2(shape, 1 - axis))

    to_cols = lax.dot_general(to_b, spread(coefs, (coefs, KPAD), 1), (((0,), (0,)), ((), ())), preferred_element_type=F32)
    from_cols = lax.dot_general(from_b, spread(vecs, (vecs, KPAD), 1), (((0,), (0,)), ((), ())), preferred_element_type=F32)
    to_cols = (to_cols * 0.5).astype(BF16)
    from_cols = (from_cols * 0.5).astype(BF16)
    to_rows = mm(spread(coefs, (dh_mat.shape[2], coefs), 0), to_b).astype(BF16)
    from_rows = mm(spread(vecs, (z_mat.shape[2], vecs), 0), from_b).astype(BF16)

    def diagonal(value):
        same = iota2(value.shape, 0) % SUB == iota2(value.shape, 1) % SUB
        return jnp.where(same, value, 0.0).astype(BF16)

    def blk_step(blk, carry):
        first = blk * blk_pts
        shape = (blk_rows, points)
        pick = ones_where(iota2(shape, 0) // SUB + first == iota2(shape, 1))
        shape = (points, KPAD)
        col = iota2(shape, 1)
        pick_t = ones_where((col // SUB + first == iota2(shape, 0)) & (col < blk_rows))
        store_wide(up_mat, (blk,), diagonal(mm(pick, to_cols)))
        store_wide(dgrid_mat, (blk,), diagonal(mm(pick, from_cols)))
        store_wide(z_mat, (blk,), diagonal(mm(from_rows, pick_t)))
        store_wide(dh_mat, (blk,), diagonal(mm(to_rows, pick_t)))
        return carry

    lax.fori_loop(0, points // blk_pts, blk_step, 0)


def kernel(dims, x_hbm, g_hbm, gain_hbm, up_hbm, gate_hbm, down_hbm, to_hbm, fromt_hbm,
           out_ref, dx_ref, dup_ref, dgate_ref, ddown_ref,
           x_ref, g_ref, gain_ref, up_ref, gate_ref, down_ref, to_ref, fromt_ref, in_sem, xfull, gfull, nfull, gain_rx, gain_cols, up_t, down_t, gate_t,
           up_mat, dgrid_mat, z_mat, dh_mat, ybuf, dmbuf, slope_buf, gate_slope, half_buf, act_buf, dpre_buf, mbuf, dhbuf, dpg_buf,
           stat_buf, part, rs1, rs2_src, rs2, back_src, back_rx, wdown_acc, wup0_acc, wup1_acc, wdown_rx, wup0_rx, wup1_rx, wdown_sum, wup0_sum, wup1_sum, wdown_full, wup0_full, wup1_full,
           ag_ss, ag_rs, gain_ss, gain_rs, rs1_ss, rs1_rs, rs2_ss, rs2_rs, back_ss, back_rs, w1_ss, w1_rs, w2_ss, w2_rs):
    coefs, chan_loc, _ = x_ref.shape
    degrees = gain_ref.shape[0]
    channels = chan_loc * 4
    vec_count = channels * (coefs - 1)
    hidden = gate_ref.shape[1]
    chunks = dims['chunks']
    blk_count = up_mat.shape[0]
    blk_rows = up_mat.shape[2]
    steps = hidden // SUB // 2
    wgrad = (wdown_acc, wup0_acc, wup1_acc)
    wgrad_rx = (wdown_rx, wup0_rx, wup1_rx)
    wsum = (wdown_sum, wup0_sum, wup1_sum)
    wfull = (wdown_full, wup0_full, wup1_full)
    me = lax.axis_index('tp')
    my_dp = lax.axis_index('dp')
    sources = (g_ref, x_ref)
    fulls = (gfull, xfull)
    grad, feat = 0, 1
    dxs, outs = 0, 1
    copies = {}

    def send(key, src, dst, ssem, rsem, axis, peer):
        copy = pltpu.make_async_remote_copy(src_ref=src, dst_ref=dst, send_sem=ssem, recv_sem=rsem, device_id={axis: peer}, device_id_type=MESH)
        copy.start()
        copies[key] = copy

    def lanes_of(chunk):
        return pl.ds(chunk * LANES, LANES)

    barrier = pltpu.get_barrier_semaphore()
    for hop in (1, 2, 3):
        pl.semaphore_signal(barrier, inc=1, device_id={'tp': tp_peer(hop)}, device_id_type=MESH)
        pl.semaphore_signal(barrier, inc=1, device_id={'dp': dp_peer(hop)}, device_id_type=MESH)
    loads = []
    pairs = ((x_hbm, x_ref), (g_hbm, g_ref), (gain_hbm, gain_ref), (up_hbm, up_ref), (gate_hbm, gate_ref), (down_hbm, down_ref), (to_hbm, to_ref), (fromt_hbm, fromt_ref))
    for j, (src, dst) in enumerate(pairs):
        loads.append(pltpu.make_async_copy(src, dst, in_sem.at[j]))
        loads[j].start()
    for j in (0, 1, 2):
        loads[j].wait()
    pl.semaphore_wait(barrier, 6)

    for hop in (1, 2, 3):
        send(('gain', hop), gain_ref, gain_rx.at[hop - 1], gain_ss.at[hop - 1], gain_rs.at[hop - 1], 'tp', tp_peer(hop))
    for chunk in range(chunks):
        for arr in (feat, grad):
            for hop in (2, 1):
                send(('ag', arr, chunk, hop), sources[arr].at[:, :, lanes_of(chunk)], fulls[arr].at[chunk, :, chan_rows(me, chan_loc), :],
                     ag_ss.at[arr, chunk, hop - 1], ag_rs.at[arr, chunk, hop - 1], 'tp', tp_peer(hop))

    def relay(arr, chunk):
        copies[('ag', arr, chunk, 2)].wait_recv()
        block = fulls[arr].at[chunk, :, chan_rows(tp_peer(2), chan_loc), :]
        send(('ag', arr, chunk, 3), block, block, ag_ss.at[arr, chunk, 2], ag_rs.at[arr, chunk, 2], 'tp', tp_peer(1))

    def gathered(arr, chunk):
        copies[('ag', arr, chunk, 1)].wait_recv()
        copies[('ag', arr, chunk, 3)].wait_recv()

    for load in loads[3:]:
        load.wait()
    for chunk in range(chunks):
        for arr in (grad, feat):
            fulls[arr][chunk, :, chan_rows(me, chan_loc), :] = sources[arr][:, :, chunk * LANES:(chunk + 1) * LANES]
    build_grid_mats(to_ref, fromt_ref, up_mat, dgrid_mat, z_mat, dh_mat, dims['blk_pts'])
    for degree in range(degrees):
        up_t[degree] = up_ref[degree].astype(F32).T.astype(BF16)
        down_t[degree] = down_ref[degree].astype(F32).T.astype(BF16)
    gate_t[...] = gate_ref[...].astype(F32).T.astype(BF16)
    for buf in (ybuf, dmbuf):
        tail = 192
        buf[:, tail:, :] = jnp.zeros((buf.shape[0], KPAD - tail, LANES), BF16)
    for acc in wgrad:
        acc[...] = jnp.zeros_like(acc)
    back_src[...] = jnp.zeros_like(back_src)

    def gain_block(tp, rows):
        eye = iota2((chan_loc, chan_loc), 0) == iota2((chan_loc, chan_loc), 1)
        for degree in range(degrees):
            col = jnp.sum(jnp.where(eye, rows[degree:degree + 1, :], 0.0), axis=1, keepdims=True)
            gain_cols[degree, chan_rows(tp, chan_loc), :] = jnp.broadcast_to(col, (chan_loc, LANES))

    gain_block(me, gain_ref[...])

    def normalize(chunk):
        scalar = xfull[chunk, 0].astype(F32)
        mean = jnp.sum(scalar, axis=0, keepdims=True) / channels
        centered = scalar - mean
        inv_s = lax.rsqrt(jnp.sum(centered * centered, axis=0, keepdims=True) / channels + NORM_EPS)
        squares = jnp.zeros((channels, LANES), F32)
        for coef in range(1, coefs):
            vec = xfull[chunk, coef].astype(F32)
            squares = squares + vec * vec
        inv_v = lax.rsqrt(jnp.sum(squares, axis=0, keepdims=True) / vec_count + NORM_EPS)
        stat_buf[chunk, 0:1, :] = mean
        stat_buf[chunk, 1:2, :] = inv_s
        stat_buf[chunk, 2:3, :] = inv_v
        nfull[chunk, 0] = (centered * inv_s * gain_cols[0]).astype(BF16)
        for degree in range(1, degrees):
            for coef in degree_span(degree):
                nfull[chunk, coef] = (xfull[chunk, coef].astype(F32) * inv_v * gain_cols[degree]).astype(BF16)

    def step_rhs(ref, idx):
        return jnp.concatenate([ref[2 * idx], ref[2 * idx + 1]], axis=1)

    def silu_pair(half):
        tan = jnp.tanh(half)
        wide = 1.0 + tan
        act = half * wide
        return act, wide + act * (1.0 - tan)

    def hidden_part(chunk):
        hid = split_coefs([mm(up_t[degree], lane_cat(nfull, chunk, degree)) for degree in range(degrees)])
        hid.append(jnp.zeros_like(hid[0]))
        for pair in range((coefs + 1) // 2):
            ybuf[:, 16 * pair:16 * pair + 16, :] = pair_rows(hid[2 * pair], hid[2 * pair + 1])
        act, slope = silu_pair(rounded(mm(gate_t[...], nfull[chunk, 0])) * 0.5)
        mbuf[chunk, 0] = act.astype(BF16)
        gate_slope[...] = 0.5 * slope

    def grad_part(chunk):
        d_mixed = split_coefs([mm(down_ref[degree], lane_cat(gfull, chunk, degree)) for degree in range(degrees)])
        dpg_buf[chunk] = (rounded(d_mixed[0]) * gate_slope[...]).astype(BF16)
        for pair in range((coefs - 1) // 2):
            dmbuf[:, 16 * pair:16 * pair + 16, :] = pair_rows(d_mixed[2 * pair + 1], d_mixed[2 * pair + 2])

    def to_points(idx, blk):
        store_wide(half_buf, (blk,), mm(load_wide(up_mat, (blk,)), step_rhs(ybuf, idx)).astype(BF16))

    def on_points(idx, blk):
        act, slope = silu_pair(load_wide(half_buf, (blk,)).astype(F32))
        store_wide(act_buf, (blk,), act.astype(BF16))
        store_wide(slope_buf, (idx, blk), slope)

    def grad_points(idx, blk):
        d_half = rounded(mm(load_wide(dgrid_mat, (blk,)), step_rhs(dmbuf, idx)))
        store_wide(dpre_buf, (blk,), (d_half * load_wide(slope_buf, (idx, blk))).astype(BF16))

    def from_points(mat, buf, blk):
        pad = jnp.zeros((KPAD - blk_rows, 2 * LANES), BF16)
        return mm(load_wide(mat, (blk,)), jnp.concatenate([load_wide(buf, (blk,)), pad], axis=0))

    def store_coefs(dst, chunk, first, idx, value):
        count = coefs - first
        value = value[:count * SUB].reshape(count, SUB, 2 * LANES)
        rows = pl.ds(pl.multiple_of(16 * idx, 16), 16)
        dst[chunk, first:coefs, rows, :] = jnp.concatenate([value[:, :, :LANES], value[:, :, LANES:]], axis=1).astype(BF16)

    def forward_turn(chunk, idx, front, mid, back):
        total = None
        for blk in range(blk_count):
            if back:
                add = from_points(z_mat, act_buf, blk)
                total = add if total is None else total + add
            if mid:
                on_points(idx - 1, blk)
            if front:
                to_points(idx, blk)
        if back:
            store_coefs(mbuf, chunk, 1, idx - 2, total)

    def backward_turn(chunk, idx, front, back):
        total = None
        for blk in range(blk_count):
            if back:
                add = from_points(dh_mat, dpre_buf, blk)
                total = add if total is None else total + add
            if front:
                grad_points(idx, blk)
        if back:
            store_coefs(dhbuf, chunk, 0, idx - 1, total)

    def loop(turn, first, last):
        def body(idx, carry):
            turn(idx)
            return carry

        lax.fori_loop(first, last, body, 0)

    def forward_grid(chunk, between):
        full = functools.partial(forward_turn, chunk, front=True, mid=True, back=True)
        forward_turn(chunk, 0, True, False, False)
        forward_turn(chunk, 1, True, True, False)
        loop(full, 2, steps // 2 + 1)
        between()
        loop(full, steps // 2 + 1, steps)
        forward_turn(chunk, steps, False, True, True)
        forward_turn(chunk, steps + 1, False, False, True)

    def backward_grid(chunk, between):
        full = functools.partial(backward_turn, chunk, front=True, back=True)
        backward_turn(chunk, 0, True, False)
        loop(full, 1, steps // 2 + 1)
        between()
        loop(full, steps // 2 + 1, steps)
        backward_turn(chunk, steps, False, True)

    def down_grads(chunk):
        for degree in range(degrees):
            rows = pl.ds(degree * hidden, hidden)
            wgrad[0][rows, :] += mm_nt(lane_cat(mbuf, chunk, degree), lane_cat(gfull, chunk, degree))

    def up_grads(chunk, half):
        rows = slice(half * hidden // 2, (half + 1) * hidden // 2)
        mats = []
        for degree in range(degrees):
            d_hid = [dhbuf[chunk, coef, rows, :] for coef in degree_span(degree)]
            d_hid = d_hid[0] if len(d_hid) == 1 else jnp.concatenate(d_hid, axis=1)
            mats.append(mm_nt(lane_cat(nfull, chunk, degree), d_hid))
        mats.append(mm_nt(nfull[chunk, 0], dpg_buf[chunk, rows, :]))
        for pair in range(len(mats) // 2):
            wgrad[1 + half][pl.ds(pair * channels, channels), :] += jnp.concatenate(mats[2 * pair:2 * pair + 2], axis=1)

    def store_part(arr, chunk, per_degree):
        for coef, value in enumerate(split_coefs(per_degree)):
            part[arr, chunk, coef] = value.astype(BF16)

    def input_grads(chunk):
        per_degree = [mm(up_ref[degree], lane_cat(dhbuf, chunk, degree)) for degree in range(degrees)]
        per_degree[0] = per_degree[0] + mm(gate_ref[...], dpg_buf[chunk])
        store_part(dxs, chunk, per_degree)

    def outputs(chunk):
        store_part(outs, chunk, [mm(down_t[degree], lane_cat(mbuf, chunk, degree)) for degree in range(degrees)])

    def scatter_core(arr, chunk):
        for chip in (0, 1):
            rows = chan_rows(2 * chip + 1 - me % 2, chan_loc)
            send(('rs1', arr, chunk, chip), part.at[arr, chunk, :, rows, :], rs1.at[arr, chunk, chip],
                 rs1_ss.at[arr, chunk, chip], rs1_rs.at[arr, chunk, chip], 'tp', tp_peer(1))

    def chip_sum(arr, chunk, chip):
        own = part[arr, chunk, :, chan_rows(2 * chip + me % 2, chan_loc), :].astype(F32)
        return own + rs1[arr, chunk, chip].astype(F32)

    def scatter_chip(arr, chunk):
        for chip in (0, 1):
            copies[('rs1', arr, chunk, chip)].wait_recv()
        rs2_src[arr, chunk] = chip_sum(arr, chunk, 1 - me // 2).astype(BF16)
        send(('rs2', arr, chunk), rs2_src.at[arr, chunk], rs2.at[arr, chunk], rs2_ss.at[arr, chunk], rs2_rs.at[arr, chunk], 'tp', tp_peer(2))

    def scattered(arr, chunk):
        copies[('rs2', arr, chunk)].wait_recv()
        return chip_sum(arr, chunk, me // 2) + rs2[arr, chunk].astype(F32)

    def own_x(chunk):
        return x_ref[:, :, chunk * LANES:(chunk + 1) * LANES].astype(F32)

    def finish_out(chunk):
        out_ref[:, :, chunk * LANES:(chunk + 1) * LANES] = (own_x(chunk) + scattered(outs, chunk)).astype(BF16)

    def own_gain(degree):
        return gain_cols[degree, chan_rows(me, chan_loc), :]

    def back_stats(chunk):
        x_own = own_x(chunk)
        d_norm = rounded(scattered(dxs, chunk))
        rs2[dxs, chunk] = d_norm.astype(BF16)
        d_hat = d_norm[0] * own_gain(0)
        hat = (x_own[0] - stat_buf[chunk, 0:1, :]) * stat_buf[chunk, 1:2, :]
        back_src[chunk, 0:1, :] = jnp.sum(d_hat, axis=0, keepdims=True)
        back_src[chunk, 1:2, :] = jnp.sum(d_hat * hat, axis=0, keepdims=True)
        total = jnp.zeros((chan_loc, LANES), F32)
        for degree in range(1, degrees):
            for coef in degree_span(degree):
                total = total + d_norm[coef] * own_gain(degree) * x_own[coef]
        back_src[chunk, 2:3, :] = jnp.sum(total, axis=0, keepdims=True)
        for hop in (2, 3, 1):
            send(('back', chunk, hop), back_src.at[chunk], back_rx.at[chunk, hop - 1], back_ss.at[chunk, hop - 1], back_rs.at[chunk, hop - 1], 'tp', tp_peer(hop))

    def finish_dx(chunk):
        for hop in (1, 2, 3):
            copies[('back', chunk, hop)].wait_recv()
        sums = (back_src[chunk] + back_rx[chunk, 0]) + (back_rx[chunk, 1] + back_rx[chunk, 2])
        mean, inv_s, inv_v = (stat_buf[chunk, j:j + 1, :] for j in range(3))
        lanes = slice(chunk * LANES, (chunk + 1) * LANES)
        hat = (x_ref[0, :, lanes].astype(F32) - mean) * inv_s
        d_hat = rs2[dxs, chunk, 0].astype(F32) * own_gain(0)
        d_scalar = inv_s * (d_hat - sums[0:1] / channels - hat * (sums[1:2] / channels))
        dx_ref[0, :, lanes] = (d_scalar + g_ref[0, :, lanes].astype(F32)).astype(BF16)
        scale = (inv_v * inv_v * inv_v) * (sums[2:3] / vec_count)
        for degree in range(1, degrees):
            for coef in degree_span(degree):
                d_hat = rs2[dxs, chunk, coef].astype(F32) * own_gain(degree)
                d_vec = inv_v * d_hat - x_ref[coef, :, lanes].astype(F32) * scale
                dx_ref[coef, :, lanes] = (d_vec + g_ref[coef, :, lanes].astype(F32)).astype(BF16)

    def quarter_rows(group, dp):
        quarter = wgrad[group].shape[0] // 4
        return pl.ds(pl.multiple_of(dp * quarter, 16), quarter)

    def wgrad_scatter(group):
        for hop in (3, 1, 2):
            send(('w1', group, hop), wgrad[group].at[quarter_rows(group, dp_peer(hop))], wgrad_rx[group].at[hop - 1],
                 w1_ss.at[group, hop - 1], w1_rs.at[group, hop - 1], 'dp', dp_peer(hop))

    def wgrad_reduce(group):
        for hop in (1, 2, 3):
            copies[('w1', group, hop)].wait_recv()
        mine = quarter_rows(group, my_dp)
        got = wgrad_rx[group]
        total = ((wgrad[group][mine, :] + got[0]) + (got[1] + got[2])).astype(BF16)
        wsum[group][...] = total
        wfull[group][mine, :] = total
        for hop in (3, 1, 2):
            send(('w2', group, hop), wsum[group], wfull[group].at[mine], w2_ss.at[group, hop - 1], w2_rs.at[group, hop - 1], 'dp', dp_peer(hop))

    def wgrad_finish(group):
        for hop in (1, 2, 3):
            copies[('w2', group, hop)].wait_recv()

    def wgrad_store():
        ddown_ref[...] = wfull[0][...]
        for mat in range(degrees + 1):
            rows = slice(mat // 2 * channels, (mat // 2 + 1) * channels)
            lanes = slice(mat % 2 * hidden // 2, (mat % 2 + 1) * hidden // 2)
            value = jnp.concatenate([wfull[1][rows, lanes], wfull[2][rows, lanes]], axis=1)
            if mat < degrees:
                dup_ref[mat * channels:(mat + 1) * channels, :] = value
            else:
                dgate_ref[...] = value

    relay(feat, 0)
    for hop in (1, 2, 3):
        copies[('gain', hop)].wait_recv()
        gain_block(tp_peer(hop), gain_rx[hop - 1])
    gathered(feat, 0)
    normalize(0)
    hidden_part(0)
    forward_grid(0, lambda: relay(grad, 0))
    outputs(0)
    scatter_core(outs, 0)
    gathered(grad, 0)
    grad_part(0)

    def between_a():
        scatter_chip(outs, 0)
        relay(feat, 1)

    backward_grid(0, between_a)
    input_grads(0)
    scatter_core(dxs, 0)
    down_grads(0)
    up_grads(0, 0)
    up_grads(0, 1)
    gathered(feat, 1)
    normalize(1)
    scatter_chip(dxs, 0)
    hidden_part(1)
    forward_grid(1, lambda: relay(grad, 1))
    outputs(1)
    scatter_core(outs, 1)
    gathered(grad, 1)
    grad_part(1)
    down_grads(1)
    wgrad_scatter(0)
    scatter_chip(outs, 1)

    def between_b():
        up_grads(1, 0)
        wgrad_scatter(1)

    backward_grid(1, between_b)
    input_grads(1)
    scatter_core(dxs, 1)
    up_grads(1, 1)
    wgrad_scatter(2)
    scatter_chip(dxs, 1)
    wgrad_reduce(0)
    wgrad_reduce(1)
    back_stats(0)
    finish_out(0)
    finish_out(1)
    wgrad_reduce(2)
    finish_dx(0)
    back_stats(1)
    for group in range(3):
        wgrad_finish(group)
    wgrad_store()
    finish_dx(1)
    for copy in copies.values():
        copy.wait_send()


def hand_on(*refs):
    count = len(refs) // 2
    for src, dst in zip(refs[:count], refs[count:]):
        dst[...] = src[...]


def solution(mesh):
    act_spec = P('dp', None, 'tp')
    in_specs = (act_spec, P(None, 'tp'), P(None, None, 'tp'), P(None, 'tp'), P(None, 'tp', None), P(None, None), P(None, None), act_spec)
    out_specs = (act_spec, act_spec, P(None, None, 'tp'), P(None, 'tp'), P(None, 'tp', None))

    def local_step(x_loc, gain_loc, up_loc, gate_loc, down_loc, to_grid, from_grid, grad_loc):
        nodes, coefs, chan_loc = x_loc.shape
        degrees, channels, hidden = up_loc.shape
        points = to_grid.shape[1]
        blk_pts = 28
        blks = points // blk_pts
        chunks = nodes // LANES
        groups = hidden // SUB
        w_rows = (degrees * hidden, (degrees + 1) * channels // 2, (degrees + 1) * channels // 2)
        dma = pltpu.SemaphoreType.DMA

        def vm(*shape, dtype=BF16):
            return pltpu.VMEM(shape, dtype)

        full = (chunks, coefs, channels, LANES)
        ins = (x_loc.transpose(1, 2, 0), grad_loc.transpose(1, 2, 0), gain_loc, up_loc, gate_loc, down_loc, to_grid, from_grid.T)
        scratch = [vm(*arr.shape, dtype=arr.dtype) for arr in ins] + [
            dma((len(ins),)), vm(*full), vm(*full), vm(*full),
            vm(3, degrees, chan_loc, dtype=F32), vm(degrees, channels, LANES, dtype=F32),
            vm(degrees, hidden, channels), vm(degrees, channels, hidden), vm(hidden, channels),
            vm(blks, 2, blk_pts * SUB, LANES), vm(blks, 2, blk_pts * SUB, LANES), vm(blks, 2, (coefs - 1) * SUB, LANES), vm(blks, 2, (coefs + 1) * SUB, LANES),
            vm(groups, KPAD, LANES), vm(groups, KPAD, LANES), vm(groups // 2, blks, 2, blk_pts * SUB, LANES, dtype=F32),
            vm(hidden, LANES, dtype=F32), vm(blks, 2, blk_pts * SUB, LANES), vm(blks, 2, blk_pts * SUB, LANES), vm(blks, 2, blk_pts * SUB, LANES), vm(chunks, coefs, hidden, LANES), vm(chunks, coefs, hidden, LANES), vm(chunks, hidden, LANES),
            vm(chunks, SUB, LANES, dtype=F32),
            vm(2, *full), vm(2, chunks, 2, coefs, chan_loc, LANES), vm(2, chunks, coefs, chan_loc, LANES), vm(2, chunks, coefs, chan_loc, LANES),
            vm(chunks, SUB, LANES, dtype=F32), vm(chunks, 3, SUB, LANES, dtype=F32),
            *(vm(rows, LANES, dtype=F32) for rows in w_rows), *(vm(3, rows // 4, LANES, dtype=F32) for rows in w_rows),
            *(vm(rows // 4, LANES) for rows in w_rows), *(vm(rows, LANES) for rows in w_rows),
            dma((2, chunks, 3)), dma((2, chunks, 3)), dma((3,)), dma((3,)),
            dma((2, chunks, 2)), dma((2, chunks, 2)), dma((2, chunks)), dma((2, chunks)),
            dma((chunks, 3)), dma((chunks, 3)), dma((3, 3)), dma((3, 3)), dma((3, 3)), dma((3, 3)),
        ]
        vmem = pl.BlockSpec(memory_space=pltpu.VMEM)
        act = jax.ShapeDtypeStruct((coefs, chan_loc, nodes), BF16)
        shapes = (act, act, jax.ShapeDtypeStruct((degrees * channels, hidden), BF16), jax.ShapeDtypeStruct((channels, hidden), BF16), jax.ShapeDtypeStruct((degrees * hidden, channels), BF16))
        results = pl.pallas_call(
            functools.partial(kernel, {'chunks': chunks, 'blk_pts': blk_pts}),
            out_shape=shapes,
            in_specs=[pl.BlockSpec(memory_space=pl.ANY)] * len(ins),
            out_specs=(vmem,) * 5,
            scratch_shapes=scratch,
            compiler_params=pltpu.CompilerParams(collective_id=0, has_side_effects=True, vmem_limit_bytes=62 * 1024 * 1024),
            name='s2_ffn',
        )(*ins)
        out_t, dx_t, d_up, d_gate, d_down = pl.pallas_call(
            hand_on,
            out_shape=shapes,
            in_specs=[vmem] * 5,
            out_specs=(vmem,) * 5,
            compiler_params=pltpu.CompilerParams(vmem_limit_bytes=62 * 1024 * 1024),
            name='hand_on',
        )(*results)
        return (out_t.transpose(2, 0, 1), dx_t.transpose(2, 0, 1), d_up.reshape(degrees, channels, hidden), d_gate, d_down.reshape(degrees, hidden, channels))

    return jax.shard_map(local_step, mesh=mesh, in_specs=in_specs, out_specs=out_specs, check_vma=False)
```

```python
import functools
import math
import jax
import jax.numpy as jnp
from jax import lax
from jax.experimental import pallas as pl
from jax.experimental.pallas import tpu as pltpu
from jax.sharding import PartitionSpec as P

NORM_EPS = 1e-5
F32 = jnp.float32
BF16 = jnp.bfloat16
MESH = pl.DeviceIdType.MESH
LANES = 128
SUB = 8
KPAD = 256


def mm(lhs, rhs):
    return jnp.dot(lhs, rhs, preferred_element_type=F32)


def mm_nt(lhs, rhs):
    return lax.dot_general(lhs, rhs, (((1,), (1,)), ((), ())), preferred_element_type=F32)


def degree_span(degree):
    return range(degree * degree, (degree + 1) * (degree + 1))


def lane_cat(ref, chunk, degree):
    parts = [ref[chunk, coef] for coef in degree_span(degree)]
    return parts[0] if len(parts) == 1 else jnp.concatenate(parts, axis=1)


def pair_rows(first, second):
    groups = first.shape[0] // SUB
    shape = (groups, SUB, first.shape[1])
    return jnp.concatenate([first.reshape(shape), second.reshape(shape)], axis=1).astype(BF16)


def split_coefs(per_degree):
    out = []
    for degree, value in enumerate(per_degree):
        out += [value[:, LANES * j:LANES * (j + 1)] for j in range(2 * degree + 1)]
    return out


def rounded(value):
    return value.astype(BF16).astype(F32)


def iota2(shape, axis):
    return lax.broadcasted_iota(jnp.int32, shape, axis)


def ones_where(cond):
    return jnp.where(cond, 1.0, 0.0).astype(BF16)


def dp_peer(hop):
    dp = lax.axis_index('dp')
    zpos, ypos = dp // 2, dp % 2
    if hop % 2:
        ypos = 1 - ypos
    if hop // 2:
        zpos = 1 - zpos
    return zpos * 2 + ypos


def tp_peer(hop):
    tp = lax.axis_index('tp')
    xpos, core = tp // 2, tp % 2
    if hop % 2:
        core = 1 - core
    if hop // 2:
        xpos = 1 - xpos
    return xpos * 2 + core


def chan_rows(tp, chan_loc):
    return pl.ds(pl.multiple_of(tp * chan_loc, chan_loc), chan_loc)


def load_wide(ref, index):
    return jnp.concatenate([ref[index + (0,)], ref[index + (1,)]], axis=1)


def store_wide(ref, index, value):
    ref[index + (0,)] = value[:, :LANES]
    ref[index + (1,)] = value[:, LANES:]


def build_grid_mats(to_ref, fromt_ref, up_mat, dgrid_mat, z_mat, dh_mat, blk_pts):
    coefs, points = to_ref.shape
    vecs = fromt_ref.shape[0]
    blk_rows = blk_pts * SUB
    to_b = to_ref[...].astype(BF16)
    from_b = fromt_ref[...].astype(BF16)

    def spread(count, shape, axis):
        return ones_where(iota2(shape, axis) // SUB == iota2(shape, 1 - axis))

    to_cols = lax.dot_general(to_b, spread(coefs, (coefs, KPAD), 1), (((0,), (0,)), ((), ())), preferred_element_type=F32)
    from_cols = lax.dot_general(from_b, spread(vecs, (vecs, KPAD), 1), (((0,), (0,)), ((), ())), preferred_element_type=F32)
    to_cols = (to_cols * 0.5).astype(BF16)
    from_cols = (from_cols * 0.5).astype(BF16)
    to_rows = mm(spread(coefs, (dh_mat.shape[2], coefs), 0), to_b).astype(BF16)
    from_rows = mm(spread(vecs, (z_mat.shape[2], vecs), 0), from_b).astype(BF16)

    def diagonal(value):
        same = iota2(value.shape, 0) % SUB == iota2(value.shape, 1) % SUB
        return jnp.where(same, value, 0.0).astype(BF16)

    def blk_step(blk, carry):
        first = blk * blk_pts
        shape = (blk_rows, points)
        pick = ones_where(iota2(shape, 0) // SUB + first == iota2(shape, 1))
        shape = (points, KPAD)
        col = iota2(shape, 1)
        pick_t = ones_where((col // SUB + first == iota2(shape, 0)) & (col < blk_rows))
        store_wide(up_mat, (blk,), diagonal(mm(pick, to_cols)))
        store_wide(dgrid_mat, (blk,), diagonal(mm(pick, from_cols)))
        store_wide(z_mat, (blk,), diagonal(mm(from_rows, pick_t)))
        store_wide(dh_mat, (blk,), diagonal(mm(to_rows, pick_t)))
        return carry

    lax.fori_loop(0, points // blk_pts, blk_step, 0)


def kernel(dims, x_hbm, g_hbm, gain_hbm, up_hbm, gate_hbm, down_hbm, to_hbm, fromt_hbm,
           out_ref, dx_ref, dup_ref, dgate_ref, ddown_ref,
           x_ref, g_ref, gain_ref, up_ref, gate_ref, down_ref, to_ref, fromt_ref, in_sem, xfull, gfull, nfull, gain_rx, gain_cols, up_t, down_t, gate_t,
           up_mat, dgrid_mat, z_mat, dh_mat, ybuf, dmbuf, slope_buf, gate_slope, half_buf, act_buf, dpre_buf, mbuf, dhbuf, dpg_buf,
           stat_buf, part, rs1, rs2_src, rs2, back_src, back_rx, wdown_acc, wup0_acc, wup1_acc, wdown_rx, wup0_rx, wup1_rx, wdown_sum, wup0_sum, wup1_sum, wdown_full, wup0_full, wup1_full,
           ag_ss, ag_rs, gain_ss, gain_rs, rs1_ss, rs1_rs, rs2_ss, rs2_rs, back_ss, back_rs, w1_ss, w1_rs, w2_ss, w2_rs):
    coefs, chan_loc, _ = x_ref.shape
    degrees = gain_ref.shape[0]
    channels = chan_loc * 4
    vec_count = channels * (coefs - 1)
    hidden = gate_ref.shape[1]
    chunks = dims['chunks']
    blk_count = up_mat.shape[0]
    blk_rows = up_mat.shape[2]
    steps = hidden // SUB // 2
    wgrad = (wdown_acc, wup0_acc, wup1_acc)
    wgrad_rx = (wdown_rx, wup0_rx, wup1_rx)
    wsum = (wdown_sum, wup0_sum, wup1_sum)
    wfull = (wdown_full, wup0_full, wup1_full)
    me = lax.axis_index('tp')
    my_dp = lax.axis_index('dp')
    sources = (g_ref, x_ref)
    fulls = (gfull, xfull)
    grad, feat = 0, 1
    dxs, outs = 0, 1
    copies = {}

    def send(key, src, dst, ssem, rsem, axis, peer):
        copy = pltpu.make_async_remote_copy(src_ref=src, dst_ref=dst, send_sem=ssem, recv_sem=rsem, device_id={axis: peer}, device_id_type=MESH)
        copy.start()
        copies[key] = copy

    def lanes_of(chunk):
        return pl.ds(chunk * LANES, LANES)

    barrier = pltpu.get_barrier_semaphore()
    for hop in (1, 2, 3):
        pl.semaphore_signal(barrier, inc=1, device_id={'tp': tp_peer(hop)}, device_id_type=MESH)
        pl.semaphore_signal(barrier, inc=1, device_id={'dp': dp_peer(hop)}, device_id_type=MESH)
    loads = []
    pairs = ((x_hbm, x_ref), (g_hbm, g_ref), (gain_hbm, gain_ref), (up_hbm, up_ref), (gate_hbm, gate_ref), (down_hbm, down_ref), (to_hbm, to_ref), (fromt_hbm, fromt_ref))
    for j, (src, dst) in enumerate(pairs):
        loads.append(pltpu.make_async_copy(src, dst, in_sem.at[j]))
        loads[j].start()
    for j in (0, 1, 2):
        loads[j].wait()
    pl.semaphore_wait(barrier, 6)

    for hop in (1, 2, 3):
        send(('gain', hop), gain_ref, gain_rx.at[hop - 1], gain_ss.at[hop - 1], gain_rs.at[hop - 1], 'tp', tp_peer(hop))
    for chunk in range(chunks):
        for arr in (feat, grad):
            for hop in (2, 1):
                send(('ag', arr, chunk, hop), sources[arr].at[:, :, lanes_of(chunk)], fulls[arr].at[chunk, :, chan_rows(me, chan_loc), :],
                     ag_ss.at[arr, chunk, hop - 1], ag_rs.at[arr, chunk, hop - 1], 'tp', tp_peer(hop))

    def relay(arr, chunk):
        copies[('ag', arr, chunk, 2)].wait_recv()
        block = fulls[arr].at[chunk, :, chan_rows(tp_peer(2), chan_loc), :]
        send(('ag', arr, chunk, 3), block, block, ag_ss.at[arr, chunk, 2], ag_rs.at[arr, chunk, 2], 'tp', tp_peer(1))

    def gathered(arr, chunk):
        copies[('ag', arr, chunk, 1)].wait_recv()
        copies[('ag', arr, chunk, 3)].wait_recv()

    for load in loads[3:]:
        load.wait()
    for chunk in range(chunks):
        for arr in (grad, feat):
            fulls[arr][chunk, :, chan_rows(me, chan_loc), :] = sources[arr][:, :, chunk * LANES:(chunk + 1) * LANES]
    build_grid_mats(to_ref, fromt_ref, up_mat, dgrid_mat, z_mat, dh_mat, dims['blk_pts'])
    for degree in range(degrees):
        up_t[degree] = up_ref[degree].astype(F32).T.astype(BF16)
        down_t[degree] = down_ref[degree].astype(F32).T.astype(BF16)
    gate_t[...] = gate_ref[...].astype(F32).T.astype(BF16)
    for buf in (ybuf, dmbuf):
        tail = 192
        buf[:, tail:, :] = jnp.zeros((buf.shape[0], KPAD - tail, LANES), BF16)
    for acc in wgrad:
        acc[...] = jnp.zeros_like(acc)
    back_src[...] = jnp.zeros_like(back_src)

    def gain_block(tp, rows):
        eye = iota2((chan_loc, chan_loc), 0) == iota2((chan_loc, chan_loc), 1)
        for degree in range(degrees):
            col = jnp.sum(jnp.where(eye, rows[degree:degree + 1, :], 0.0), axis=1, keepdims=True)
            gain_cols[degree, chan_rows(tp, chan_loc), :] = jnp.broadcast_to(col, (chan_loc, LANES))

    gain_block(me, gain_ref[...])

    def normalize(chunk):
        scalar = xfull[chunk, 0].astype(F32)
        mean = jnp.sum(scalar, axis=0, keepdims=True) / channels
        centered = scalar - mean
        inv_s = lax.rsqrt(jnp.sum(centered * centered, axis=0, keepdims=True) / channels + NORM_EPS)
        squares = jnp.zeros((channels, LANES), F32)
        for coef in range(1, coefs):
            vec = xfull[chunk, coef].astype(F32)
            squares = squares + vec * vec
        inv_v = lax.rsqrt(jnp.sum(squares, axis=0, keepdims=True) / vec_count + NORM_EPS)
        stat_buf[chunk, 0:1, :] = mean
        stat_buf[chunk, 1:2, :] = inv_s
        stat_buf[chunk, 2:3, :] = inv_v
        nfull[chunk, 0] = (centered * inv_s * gain_cols[0]).astype(BF16)
        for degree in range(1, degrees):
            for coef in degree_span(degree):
                nfull[chunk, coef] = (xfull[chunk, coef].astype(F32) * inv_v * gain_cols[degree]).astype(BF16)

    def step_rhs(ref, idx):
        return jnp.concatenate([ref[2 * idx], ref[2 * idx + 1]], axis=1)

    def silu_pair(half):
        tan = jnp.tanh(half)
        wide = 1.0 + tan
        act = half * wide
        return act, wide + act * (1.0 - tan)

    def hidden_part(chunk):
        hid = split_coefs([mm(up_t[degree], lane_cat(nfull, chunk, degree)) for degree in range(degrees)])
        hid.append(jnp.zeros_like(hid[0]))
        for pair in range((coefs + 1) // 2):
            ybuf[:, 16 * pair:16 * pair + 16, :] = pair_rows(hid[2 * pair], hid[2 * pair + 1])
        act, slope = silu_pair(rounded(mm(gate_t[...], nfull[chunk, 0])) * 0.5)
        mbuf[chunk, 0] = act.astype(BF16)
        gate_slope[...] = 0.5 * slope

    def grad_part(chunk):
        d_mixed = split_coefs([mm(down_ref[degree], lane_cat(gfull, chunk, degree)) for degree in range(degrees)])
        dpg_buf[chunk] = (rounded(d_mixed[0]) * gate_slope[...]).astype(BF16)
        for pair in range((coefs - 1) // 2):
            dmbuf[:, 16 * pair:16 * pair + 16, :] = pair_rows(d_mixed[2 * pair + 1], d_mixed[2 * pair + 2])

    def to_points(idx, blk):
        store_wide(half_buf, (blk,), mm(load_wide(up_mat, (blk,)), step_rhs(ybuf, idx)).astype(BF16))

    def on_points(idx, blk):
        act, slope = silu_pair(load_wide(half_buf, (blk,)).astype(F32))
        store_wide(act_buf, (blk,), act.astype(BF16))
        store_wide(slope_buf, (idx, blk), slope)

    def grad_points(idx, blk):
        d_half = rounded(mm(load_wide(dgrid_mat, (blk,)), step_rhs(dmbuf, idx)))
        store_wide(dpre_buf, (blk,), (d_half * load_wide(slope_buf, (idx, blk))).astype(BF16))

    def from_points(mat, buf, blk):
        pad = jnp.zeros((KPAD - blk_rows, 2 * LANES), BF16)
        return mm(load_wide(mat, (blk,)), jnp.concatenate([load_wide(buf, (blk,)), pad], axis=0))

    def store_coefs(dst, chunk, first, idx, value):
        count = coefs - first
        value = value[:count * SUB].reshape(count, SUB, 2 * LANES)
        rows = pl.ds(pl.multiple_of(16 * idx, 16), 16)
        dst[chunk, first:coefs, rows, :] = jnp.concatenate([value[:, :, :LANES], value[:, :, LANES:]], axis=1).astype(BF16)

    def forward_turn(chunk, idx, front, mid, back):
        total = None
        for blk in range(blk_count):
            if back:
                add = from_points(z_mat, act_buf, blk)
                total = add if total is None else total + add
            if mid:
                on_points(idx - 1, blk)
            if front:
                to_points(idx, blk)
        if back:
            store_coefs(mbuf, chunk, 1, idx - 2, total)

    def backward_turn(chunk, idx, front, back):
        total = None
        for blk in range(blk_count):
            if back:
                add = from_points(dh_mat, dpre_buf, blk)
                total = add if total is None else total + add
            if front:
                grad_points(idx, blk)
        if back:
            store_coefs(dhbuf, chunk, 0, idx - 1, total)

    def loop(turn, first, last):
        def body(trip, carry):
            turn(first + 2 * trip)
            turn(first + 2 * trip + 1)
            return carry

        lax.fori_loop(0, (last - first) // 2, body, 0)

    def forward_grid(chunk, between, last):
        full = functools.partial(forward_turn, chunk, front=True, mid=True, back=True)
        split = steps - 4
        forward_turn(chunk, 0, True, False, False)
        forward_turn(chunk, 1, True, True, False)
        loop(full, 2, split)
        between()
        loop(full, split, steps)
        last()
        forward_turn(chunk, steps, False, True, True)
        forward_turn(chunk, steps + 1, False, False, True)
        backward_turn(chunk, 0, True, False)

    def backward_grid(chunk, between, last):
        full = functools.partial(backward_turn, chunk, front=True, back=True)
        split = steps // 2 + 1
        loop(full, 1, split)
        between()
        loop(full, split, steps - 1)
        last()
        full(steps - 1)
        backward_turn(chunk, steps, False, True)

    def down_grads(chunk):
        for degree in range(degrees):
            rows = pl.ds(degree * hidden, hidden)
            wgrad[0][rows, :] += mm_nt(lane_cat(mbuf, chunk, degree), lane_cat(gfull, chunk, degree))

    def up_grads(chunk, half):
        rows = slice(half * hidden // 2, (half + 1) * hidden // 2)
        mats = []
        for degree in range(degrees):
            d_hid = [dhbuf[chunk, coef, rows, :] for coef in degree_span(degree)]
            d_hid = d_hid[0] if len(d_hid) == 1 else jnp.concatenate(d_hid, axis=1)
            mats.append(mm_nt(lane_cat(nfull, chunk, degree), d_hid))
        mats.append(mm_nt(nfull[chunk, 0], dpg_buf[chunk, rows, :]))
        for pair in range(len(mats) // 2):
            wgrad[1 + half][pl.ds(pair * channels, channels), :] += jnp.concatenate(mats[2 * pair:2 * pair + 2], axis=1)

    def store_part(arr, chunk, per_degree):
        for coef, value in enumerate(split_coefs(per_degree)):
            part[arr, chunk, coef] = value.astype(BF16)

    def input_grads(chunk):
        per_degree = [mm(up_ref[degree], lane_cat(dhbuf, chunk, degree)) for degree in range(degrees)]
        per_degree[0] = per_degree[0] + mm(gate_ref[...], dpg_buf[chunk])
        store_part(dxs, chunk, per_degree)

    def outputs(chunk):
        store_part(outs, chunk, [mm(down_t[degree], lane_cat(mbuf, chunk, degree)) for degree in range(degrees)])

    chips = (1 - me // 2, me // 2)

    def scatter_core(arr, chunk):
        for slot, chip in enumerate(chips):
            rows = chan_rows(2 * chip + 1 - me % 2, chan_loc)
            send(('rs1', arr, chunk, slot), part.at[arr, chunk, :, rows, :], rs1.at[arr, chunk, slot],
                 rs1_ss.at[arr, chunk, slot], rs1_rs.at[arr, chunk, slot], 'tp', tp_peer(1))

    def chip_sum(arr, chunk, slot):
        copies[('rs1', arr, chunk, slot)].wait_recv()
        own = part[arr, chunk, :, chan_rows(2 * chips[slot] + me % 2, chan_loc), :].astype(F32)
        return own + rs1[arr, chunk, slot].astype(F32)

    def scatter_chip(arr, chunk):
        rs2_src[arr, chunk] = chip_sum(arr, chunk, 0).astype(BF16)
        send(('rs2', arr, chunk), rs2_src.at[arr, chunk], rs2.at[arr, chunk], rs2_ss.at[arr, chunk], rs2_rs.at[arr, chunk], 'tp', tp_peer(2))

    def scattered(arr, chunk):
        total = chip_sum(arr, chunk, 1)
        copies[('rs2', arr, chunk)].wait_recv()
        return total + rs2[arr, chunk].astype(F32)

    def own_x(chunk):
        return x_ref[:, :, chunk * LANES:(chunk + 1) * LANES].astype(F32)

    def finish_out(chunk):
        out_ref[:, :, chunk * LANES:(chunk + 1) * LANES] = (own_x(chunk) + scattered(outs, chunk)).astype(BF16)

    def own_gain(degree):
        return gain_cols[degree, chan_rows(me, chan_loc), :]

    def back_stats(chunk):
        x_own = own_x(chunk)
        d_norm = rounded(scattered(dxs, chunk))
        rs2[dxs, chunk] = d_norm.astype(BF16)
        d_hat = d_norm[0] * own_gain(0)
        hat = (x_own[0] - stat_buf[chunk, 0:1, :]) * stat_buf[chunk, 1:2, :]
        back_src[chunk, 0:1, :] = jnp.sum(d_hat, axis=0, keepdims=True)
        back_src[chunk, 1:2, :] = jnp.sum(d_hat * hat, axis=0, keepdims=True)
        total = jnp.zeros((chan_loc, LANES), F32)
        for degree in range(1, degrees):
            for coef in degree_span(degree):
                total = total + d_norm[coef] * own_gain(degree) * x_own[coef]
        back_src[chunk, 2:3, :] = jnp.sum(total, axis=0, keepdims=True)
        for hop in (2, 3, 1):
            send(('back', chunk, hop), back_src.at[chunk], back_rx.at[chunk, hop - 1], back_ss.at[chunk, hop - 1], back_rs.at[chunk, hop - 1], 'tp', tp_peer(hop))

    def finish_dx(chunk):
        for hop in (1, 2, 3):
            copies[('back', chunk, hop)].wait_recv()
        sums = (back_src[chunk] + back_rx[chunk, 0]) + (back_rx[chunk, 1] + back_rx[chunk, 2])
        mean, inv_s, inv_v = (stat_buf[chunk, j:j + 1, :] for j in range(3))
        lanes = slice(chunk * LANES, (chunk + 1) * LANES)
        hat = (x_ref[0, :, lanes].astype(F32) - mean) * inv_s
        d_hat = rs2[dxs, chunk, 0].astype(F32) * own_gain(0)
        d_scalar = inv_s * (d_hat - sums[0:1] / channels - hat * (sums[1:2] / channels))
        dx_ref[0, :, lanes] = (d_scalar + g_ref[0, :, lanes].astype(F32)).astype(BF16)
        scale = (inv_v * inv_v * inv_v) * (sums[2:3] / vec_count)
        for degree in range(1, degrees):
            for coef in degree_span(degree):
                d_hat = rs2[dxs, chunk, coef].astype(F32) * own_gain(degree)
                d_vec = inv_v * d_hat - x_ref[coef, :, lanes].astype(F32) * scale
                dx_ref[coef, :, lanes] = (d_vec + g_ref[coef, :, lanes].astype(F32)).astype(BF16)

    def quarter_rows(group, dp):
        quarter = wgrad[group].shape[0] // 4
        return pl.ds(pl.multiple_of(dp * quarter, 16), quarter)

    def wgrad_scatter(group):
        for hop in (3, 1, 2):
            send(('w1', group, hop), wgrad[group].at[quarter_rows(group, dp_peer(hop))], wgrad_rx[group].at[hop - 1],
                 w1_ss.at[group, hop - 1], w1_rs.at[group, hop - 1], 'dp', dp_peer(hop))

    def wgrad_reduce(group):
        for hop in (1, 2, 3):
            copies[('w1', group, hop)].wait_recv()
        mine = quarter_rows(group, my_dp)
        got = wgrad_rx[group]
        total = ((wgrad[group][mine, :] + got[0]) + (got[1] + got[2])).astype(BF16)
        wsum[group][...] = total
        wfull[group][mine, :] = total
        for hop in (3, 1, 2):
            send(('w2', group, hop), wsum[group], wfull[group].at[mine], w2_ss.at[group, hop - 1], w2_rs.at[group, hop - 1], 'dp', dp_peer(hop))

    def wgrad_finish(group):
        for hop in (1, 2, 3):
            copies[('w2', group, hop)].wait_recv()

    def wgrad_store():
        ddown_ref[...] = wfull[0][...]
        for mat in range(degrees + 1):
            rows = slice(mat // 2 * channels, (mat // 2 + 1) * channels)
            lanes = slice(mat % 2 * hidden // 2, (mat % 2 + 1) * hidden // 2)
            value = jnp.concatenate([wfull[1][rows, lanes], wfull[2][rows, lanes]], axis=1)
            if mat < degrees:
                dup_ref[mat * channels:(mat + 1) * channels, :] = value
            else:
                dgate_ref[...] = value

    relay(feat, 0)
    for hop in (1, 2, 3):
        copies[('gain', hop)].wait_recv()
        gain_block(tp_peer(hop), gain_rx[hop - 1])
    gathered(feat, 0)
    normalize(0)
    hidden_part(0)
    def arrived(chunk):
        gathered(grad, chunk)
        grad_part(chunk)

    forward_grid(0, lambda: relay(grad, 0), lambda: arrived(0))
    outputs(0)
    scatter_core(outs, 0)

    def between_a():
        scatter_chip(outs, 0)
        relay(feat, 1)

    def last_a():
        gathered(feat, 1)
        down_grads(0)

    backward_grid(0, between_a, last_a)
    input_grads(0)
    scatter_core(dxs, 0)
    up_grads(0, 0)
    up_grads(0, 1)
    normalize(1)
    scatter_chip(dxs, 0)
    hidden_part(1)
    forward_grid(1, lambda: relay(grad, 1), lambda: arrived(1))
    outputs(1)
    scatter_core(outs, 1)
    down_grads(1)
    wgrad_scatter(0)
    scatter_chip(outs, 1)

    def between_b():
        up_grads(1, 0)
        wgrad_scatter(1)

    backward_grid(1, between_b, lambda: None)
    input_grads(1)
    scatter_core(dxs, 1)
    up_grads(1, 1)
    wgrad_scatter(2)
    scatter_chip(dxs, 1)
    wgrad_reduce(0)
    wgrad_reduce(1)
    back_stats(0)
    finish_out(0)
    finish_out(1)
    wgrad_reduce(2)
    finish_dx(0)
    back_stats(1)
    for group in range(3):
        wgrad_finish(group)
    wgrad_store()
    finish_dx(1)
    for copy in copies.values():
        copy.wait_send()


def hand_on(*refs):
    count = (len(refs) - 2) // 3
    srcs, dsts, bufs, (in_sem, out_sem) = refs[:count], refs[count:2 * count], refs[2 * count:3 * count], refs[3 * count:]
    ins = [pltpu.make_async_copy(srcs[j], bufs[j], in_sem.at[j]) for j in range(count)]
    outs = [pltpu.make_async_copy(bufs[j], dsts[j], out_sem.at[j]) for j in range(count)]
    for copy in ins:
        copy.start()
    for j in range(count):
        ins[j].wait()
        outs[j].start()
    for copy in outs:
        copy.wait()


def solution(mesh):
    act_spec = P('dp', None, 'tp')
    in_specs = (act_spec, P(None, 'tp'), P(None, None, 'tp'), P(None, 'tp'), P(None, 'tp', None), P(None, None), P(None, None), act_spec)
    out_specs = (act_spec, act_spec, P(None, None, 'tp'), P(None, 'tp'), P(None, 'tp', None))

    def local_step(x_loc, gain_loc, up_loc, gate_loc, down_loc, to_grid, from_grid, grad_loc):
        nodes, coefs, chan_loc = x_loc.shape
        degrees, channels, hidden = up_loc.shape
        points = to_grid.shape[1]
        blk_pts = 28
        blks = points // blk_pts
        chunks = nodes // LANES
        groups = hidden // SUB
        w_rows = (degrees * hidden, (degrees + 1) * channels // 2, (degrees + 1) * channels // 2)
        dma = pltpu.SemaphoreType.DMA

        def vm(*shape, dtype=BF16):
            return pltpu.VMEM(shape, dtype)

        full = (chunks, coefs, channels, LANES)
        ins = (x_loc.transpose(1, 2, 0), grad_loc.transpose(1, 2, 0), gain_loc, up_loc, gate_loc, down_loc, to_grid, from_grid.T)
        scratch = [vm(*arr.shape, dtype=arr.dtype) for arr in ins] + [
            dma((len(ins),)), vm(*full), vm(*full), vm(*full),
            vm(3, degrees, chan_loc, dtype=F32), vm(degrees, channels, LANES, dtype=F32),
            vm(degrees, hidden, channels), vm(degrees, channels, hidden), vm(hidden, channels),
            vm(blks, 2, blk_pts * SUB, LANES), vm(blks, 2, blk_pts * SUB, LANES), vm(blks, 2, (coefs - 1) * SUB, LANES), vm(blks, 2, (coefs + 1) * SUB, LANES),
            vm(groups, KPAD, LANES), vm(groups, KPAD, LANES), vm(groups // 2, blks, 2, blk_pts * SUB, LANES, dtype=F32),
            vm(hidden, LANES, dtype=F32), vm(blks, 2, blk_pts * SUB, LANES), vm(blks, 2, blk_pts * SUB, LANES), vm(blks, 2, blk_pts * SUB, LANES), vm(chunks, coefs, hidden, LANES), vm(chunks, coefs, hidden, LANES), vm(chunks, hidden, LANES),
            vm(chunks, SUB, LANES, dtype=F32),
            vm(2, *full), vm(2, chunks, 2, coefs, chan_loc, LANES), vm(2, chunks, coefs, chan_loc, LANES), vm(2, chunks, coefs, chan_loc, LANES),
            vm(chunks, SUB, LANES, dtype=F32), vm(chunks, 3, SUB, LANES, dtype=F32),
            *(vm(rows, LANES, dtype=F32) for rows in w_rows), *(vm(3, rows // 4, LANES, dtype=F32) for rows in w_rows),
            *(vm(rows // 4, LANES) for rows in w_rows), *(vm(rows, LANES) for rows in w_rows),
            dma((2, chunks, 3)), dma((2, chunks, 3)), dma((3,)), dma((3,)),
            dma((2, chunks, 2)), dma((2, chunks, 2)), dma((2, chunks)), dma((2, chunks)),
            dma((chunks, 3)), dma((chunks, 3)), dma((3, 3)), dma((3, 3)), dma((3, 3)), dma((3, 3)),
        ]
        vmem = pl.BlockSpec(memory_space=pltpu.VMEM)
        act = jax.ShapeDtypeStruct((coefs, chan_loc, nodes), BF16)
        shapes = (act, act, jax.ShapeDtypeStruct((degrees * channels, hidden), BF16), jax.ShapeDtypeStruct((channels, hidden), BF16), jax.ShapeDtypeStruct((degrees * hidden, channels), BF16))
        results = pl.pallas_call(
            functools.partial(kernel, {'chunks': chunks, 'blk_pts': blk_pts}),
            out_shape=shapes,
            in_specs=[pl.BlockSpec(memory_space=pl.ANY)] * len(ins),
            out_specs=(vmem,) * 5,
            scratch_shapes=scratch,
            compiler_params=pltpu.CompilerParams(collective_id=0, has_side_effects=True, vmem_limit_bytes=62 * 1024 * 1024),
            name='s2_ffn',
        )(*ins)
        out_t, dx_t, d_up, d_gate, d_down = pl.pallas_call(
            hand_on,
            out_shape=shapes,
            in_specs=[pl.BlockSpec(memory_space=pl.ANY)] * len(shapes),
            out_specs=(pl.BlockSpec(memory_space=pl.ANY),) * len(shapes),
            scratch_shapes=[vm(*arr.shape) for arr in shapes] + [dma((len(shapes),)), dma((len(shapes),))],
            compiler_params=pltpu.CompilerParams(vmem_limit_bytes=62 * 1024 * 1024),
            name='hand_on',
        )(*results)
        return (out_t.transpose(2, 0, 1), dx_t.transpose(2, 0, 1), d_up.reshape(degrees, channels, hidden), d_gate, d_down.reshape(degrees, hidden, channels))

    return jax.shard_map(local_step, mesh=mesh, in_specs=in_specs, out_specs=out_specs, check_vma=False)
```

```python
import functools
import math
import jax
import jax.numpy as jnp
from jax import lax
from jax.experimental import pallas as pl
from jax.experimental.pallas import tpu as pltpu
from jax.sharding import PartitionSpec as P

NORM_EPS = 1e-5
F32 = jnp.float32
BF16 = jnp.bfloat16
MESH = pl.DeviceIdType.MESH
LANES = 128
SUB = 8
KPAD = 256


def mm(lhs, rhs):
    return jnp.dot(lhs, rhs, preferred_element_type=F32)


def mm_nt(lhs, rhs):
    return lax.dot_general(lhs, rhs, (((1,), (1,)), ((), ())), preferred_element_type=F32)


def degree_span(degree):
    return range(degree * degree, (degree + 1) * (degree + 1))


def lane_cat(ref, chunk, degree):
    parts = [ref[chunk, coef] for coef in degree_span(degree)]
    return parts[0] if len(parts) == 1 else jnp.concatenate(parts, axis=1)


def pair_rows(first, second):
    groups = first.shape[0] // SUB
    shape = (groups, SUB, first.shape[1])
    return jnp.concatenate([first.reshape(shape), second.reshape(shape)], axis=1).astype(BF16)


def split_coefs(per_degree):
    out = []
    for degree, value in enumerate(per_degree):
        out += [value[:, LANES * j:LANES * (j + 1)] for j in range(2 * degree + 1)]
    return out


def rounded(value):
    return value.astype(BF16).astype(F32)


def iota2(shape, axis):
    return lax.broadcasted_iota(jnp.int32, shape, axis)


def ones_where(cond):
    return jnp.where(cond, 1.0, 0.0).astype(BF16)


def dp_peer(hop):
    dp = lax.axis_index('dp')
    zpos, ypos = dp // 2, dp % 2
    if hop % 2:
        ypos = 1 - ypos
    if hop // 2:
        zpos = 1 - zpos
    return zpos * 2 + ypos


def tp_peer(hop):
    tp = lax.axis_index('tp')
    xpos, core = tp // 2, tp % 2
    if hop % 2:
        core = 1 - core
    if hop // 2:
        xpos = 1 - xpos
    return xpos * 2 + core


def chan_rows(tp, chan_loc):
    return pl.ds(pl.multiple_of(tp * chan_loc, chan_loc), chan_loc)


def load_wide(ref, index):
    return jnp.concatenate([ref[index + (0,)], ref[index + (1,)]], axis=1)


def store_wide(ref, index, value):
    ref[index + (0,)] = value[:, :LANES]
    ref[index + (1,)] = value[:, LANES:]


def build_grid_mats(to_ref, fromt_ref, up_mat, dgrid_mat, z_mat, dh_mat, blk_pts):
    coefs, points = to_ref.shape
    vecs = fromt_ref.shape[0]
    blk_rows = blk_pts * SUB
    to_b = to_ref[...].astype(BF16)
    from_b = fromt_ref[...].astype(BF16)

    def spread(count, shape, axis):
        return ones_where(iota2(shape, axis) // SUB == iota2(shape, 1 - axis))

    to_cols = lax.dot_general(to_b, spread(coefs, (coefs, KPAD), 1), (((0,), (0,)), ((), ())), preferred_element_type=F32)
    from_cols = lax.dot_general(from_b, spread(vecs, (vecs, KPAD), 1), (((0,), (0,)), ((), ())), preferred_element_type=F32)
    to_cols = (to_cols * 0.5).astype(BF16)
    from_cols = (from_cols * 0.5).astype(BF16)
    to_rows = mm(spread(coefs, (dh_mat.shape[2], coefs), 0), to_b).astype(BF16)
    from_rows = mm(spread(vecs, (z_mat.shape[2], vecs), 0), from_b).astype(BF16)

    def diagonal(value):
        same = iota2(value.shape, 0) % SUB == iota2(value.shape, 1) % SUB
        return jnp.where(same, value, 0.0).astype(BF16)

    def blk_step(blk, carry):
        first = blk * blk_pts
        shape = (blk_rows, points)
        pick = ones_where(iota2(shape, 0) // SUB + first == iota2(shape, 1))
        shape = (points, KPAD)
        col = iota2(shape, 1)
        pick_t = ones_where((col // SUB + first == iota2(shape, 0)) & (col < blk_rows))
        store_wide(up_mat, (blk,), diagonal(mm(pick, to_cols)))
        store_wide(dgrid_mat, (blk,), diagonal(mm(pick, from_cols)))
        store_wide(z_mat, (blk,), diagonal(mm(from_rows, pick_t)))
        store_wide(dh_mat, (blk,), diagonal(mm(to_rows, pick_t)))
        return carry

    lax.fori_loop(0, points // blk_pts, blk_step, 0)


def kernel(dims, x_hbm, g_hbm, gain_hbm, up_hbm, gate_hbm, down_hbm, to_hbm, fromt_hbm,
           out_ref, dx_ref, dup_ref, dgate_ref, ddown_ref,
           x_ref, g_ref, gain_ref, up_ref, gate_ref, down_ref, to_ref, fromt_ref, in_sem, xfull, gfull, nfull, gain_rx, gain_cols, up_t, down_t, gate_t,
           up_mat, dgrid_mat, z_mat, dh_mat, ybuf, dmbuf, slope_buf, gate_slope, half_buf, act_buf, dpre_buf, mbuf, dhbuf, dpg_buf,
           stat_buf, part, rs1, rs2_src, rs2, back_src, back_rx, wdown_acc, wup0_acc, wup1_acc, wdown_rx, wup0_rx, wup1_rx, wdown_sum, wup0_sum, wup1_sum, wdown_full, wup0_full, wup1_full,
           ag_ss, ag_rs, gain_ss, gain_rs, rs1_ss, rs1_rs, rs2_ss, rs2_rs, back_ss, back_rs, w1_ss, w1_rs, w2_ss, w2_rs):
    coefs, chan_loc, _ = x_ref.shape
    degrees = gain_ref.shape[0]
    channels = chan_loc * 4
    vec_count = channels * (coefs - 1)
    hidden = gate_ref.shape[1]
    chunks = dims['chunks']
    blk_count = up_mat.shape[0]
    blk_rows = up_mat.shape[2]
    steps = hidden // SUB // 2
    wgrad = (wdown_acc, wup0_acc, wup1_acc)
    wgrad_rx = (wdown_rx, wup0_rx, wup1_rx)
    wsum = (wdown_sum, wup0_sum, wup1_sum)
    wfull = (wdown_full, wup0_full, wup1_full)
    me = lax.axis_index('tp')
    my_dp = lax.axis_index('dp')
    sources = (g_ref, x_ref)
    fulls = (gfull, xfull)
    grad, feat = 0, 1
    dxs, outs = 0, 1
    copies = {}

    def send(key, src, dst, ssem, rsem, axis, peer):
        copy = pltpu.make_async_remote_copy(src_ref=src, dst_ref=dst, send_sem=ssem, recv_sem=rsem, device_id={axis: peer}, device_id_type=MESH)
        copy.start()
        copies[key] = copy

    def lanes_of(chunk):
        return pl.ds(chunk * LANES, LANES)

    barrier = pltpu.get_barrier_semaphore()
    for hop in (1, 2, 3):
        pl.semaphore_signal(barrier, inc=1, device_id={'tp': tp_peer(hop)}, device_id_type=MESH)
        pl.semaphore_signal(barrier, inc=1, device_id={'dp': dp_peer(hop)}, device_id_type=MESH)
    loads = []
    pairs = ((x_hbm, x_ref), (g_hbm, g_ref), (gain_hbm, gain_ref), (up_hbm, up_ref), (gate_hbm, gate_ref), (down_hbm, down_ref), (to_hbm, to_ref), (fromt_hbm, fromt_ref))
    for j, (src, dst) in enumerate(pairs):
        loads.append(pltpu.make_async_copy(src, dst, in_sem.at[j]))
        loads[j].start()
    for j in (0, 1, 2):
        loads[j].wait()
    pl.semaphore_wait(barrier, 6)

    for hop in (1, 2, 3):
        send(('gain', hop), gain_ref, gain_rx.at[hop - 1], gain_ss.at[hop - 1], gain_rs.at[hop - 1], 'tp', tp_peer(hop))
    for chunk in range(chunks):
        for arr in (feat, grad):
            for hop in (2, 1):
                send(('ag', arr, chunk, hop), sources[arr].at[:, :, lanes_of(chunk)], fulls[arr].at[chunk, :, chan_rows(me, chan_loc), :],
                     ag_ss.at[arr, chunk, hop - 1], ag_rs.at[arr, chunk, hop - 1], 'tp', tp_peer(hop))

    def relay(arr, chunk):
        copies[('ag', arr, chunk, 2)].wait_recv()
        block = fulls[arr].at[chunk, :, chan_rows(tp_peer(2), chan_loc), :]
        send(('ag', arr, chunk, 3), block, block, ag_ss.at[arr, chunk, 2], ag_rs.at[arr, chunk, 2], 'tp', tp_peer(1))

    def gathered(arr, chunk):
        copies[('ag', arr, chunk, 1)].wait_recv()
        copies[('ag', arr, chunk, 3)].wait_recv()

    for load in loads[3:]:
        load.wait()
    for chunk in range(chunks):
        for arr in (grad, feat):
            fulls[arr][chunk, :, chan_rows(me, chan_loc), :] = sources[arr][:, :, chunk * LANES:(chunk + 1) * LANES]
    build_grid_mats(to_ref, fromt_ref, up_mat, dgrid_mat, z_mat, dh_mat, dims['blk_pts'])
    for degree in range(degrees):
        up_t[degree] = up_ref[degree].astype(F32).T.astype(BF16)
        down_t[degree] = down_ref[degree].astype(F32).T.astype(BF16)
    gate_t[...] = gate_ref[...].astype(F32).T.astype(BF16)
    for buf in (ybuf, dmbuf):
        tail = 192
        buf[:, tail:, :] = jnp.zeros((buf.shape[0], KPAD - tail, LANES), BF16)
    for acc in wgrad:
        acc[...] = jnp.zeros_like(acc)
    back_src[...] = jnp.zeros_like(back_src)

    def gain_block(tp, rows):
        eye = iota2((chan_loc, chan_loc), 0) == iota2((chan_loc, chan_loc), 1)
        for degree in range(degrees):
            col = jnp.sum(jnp.where(eye, rows[degree:degree + 1, :], 0.0), axis=1, keepdims=True)
            gain_cols[degree, chan_rows(tp, chan_loc), :] = jnp.broadcast_to(col, (chan_loc, LANES))

    gain_block(me, gain_ref[...])

    def normalize(chunk):
        scalar = xfull[chunk, 0].astype(F32)
        mean = jnp.sum(scalar, axis=0, keepdims=True) / channels
        centered = scalar - mean
        inv_s = lax.rsqrt(jnp.sum(centered * centered, axis=0, keepdims=True) / channels + NORM_EPS)
        squares = jnp.zeros((channels, LANES), F32)
        for coef in range(1, coefs):
            vec = xfull[chunk, coef].astype(F32)
            squares = squares + vec * vec
        inv_v = lax.rsqrt(jnp.sum(squares, axis=0, keepdims=True) / vec_count + NORM_EPS)
        stat_buf[chunk, 0:1, :] = mean
        stat_buf[chunk, 1:2, :] = inv_s
        stat_buf[chunk, 2:3, :] = inv_v
        nfull[chunk, 0] = (centered * inv_s * gain_cols[0]).astype(BF16)
        for degree in range(1, degrees):
            for coef in degree_span(degree):
                nfull[chunk, coef] = (xfull[chunk, coef].astype(F32) * inv_v * gain_cols[degree]).astype(BF16)

    def step_rhs(ref, idx):
        return jnp.concatenate([ref[2 * idx], ref[2 * idx + 1]], axis=1)

    def silu_pair(half):
        tan = jnp.tanh(half)
        wide = 1.0 + tan
        act = half * wide
        return act, wide + act * (1.0 - tan)

    def hidden_part(chunk):
        hid = split_coefs([mm(up_t[degree], lane_cat(nfull, chunk, degree)) for degree in range(degrees)])
        hid.append(jnp.zeros_like(hid[0]))
        for pair in range((coefs + 1) // 2):
            ybuf[:, 16 * pair:16 * pair + 16, :] = pair_rows(hid[2 * pair], hid[2 * pair + 1])
        act, slope = silu_pair(rounded(mm(gate_t[...], nfull[chunk, 0])) * 0.5)
        mbuf[chunk, 0] = act.astype(BF16)
        gate_slope[...] = 0.5 * slope

    def grad_part(chunk):
        d_mixed = split_coefs([mm(down_ref[degree], lane_cat(gfull, chunk, degree)) for degree in range(degrees)])
        dpg_buf[chunk] = (rounded(d_mixed[0]) * gate_slope[...]).astype(BF16)
        for pair in range((coefs - 1) // 2):
            dmbuf[:, 16 * pair:16 * pair + 16, :] = pair_rows(d_mixed[2 * pair + 1], d_mixed[2 * pair + 2])

    def to_points(idx, blk):
        store_wide(half_buf, (blk,), mm(load_wide(up_mat, (blk,)), step_rhs(ybuf, idx)).astype(BF16))

    def on_points(idx, blk):
        act, slope = silu_pair(load_wide(half_buf, (blk,)).astype(F32))
        store_wide(act_buf, (blk,), act.astype(BF16))
        store_wide(slope_buf, (idx, blk), slope)

    def grad_points(idx, blk):
        d_half = rounded(mm(load_wide(dgrid_mat, (blk,)), step_rhs(dmbuf, idx)))
        store_wide(dpre_buf, (blk,), (d_half * load_wide(slope_buf, (idx, blk))).astype(BF16))

    def from_points(mat, buf, blk):
        pad = jnp.zeros((KPAD - blk_rows, 2 * LANES), BF16)
        return mm(load_wide(mat, (blk,)), jnp.concatenate([load_wide(buf, (blk,)), pad], axis=0))

    def store_coefs(dst, chunk, first, idx, value):
        count = coefs - first
        value = value[:count * SUB].reshape(count, SUB, 2 * LANES)
        rows = pl.ds(pl.multiple_of(16 * idx, 16), 16)
        dst[chunk, first:coefs, rows, :] = jnp.concatenate([value[:, :, :LANES], value[:, :, LANES:]], axis=1).astype(BF16)

    def forward_turn(chunk, idx, front, mid, back):
        total = None
        for blk in range(blk_count):
            if back:
                add = from_points(z_mat, act_buf, blk)
                total = add if total is None else total + add
            if mid:
                on_points(idx - 1, blk)
            if front:
                to_points(idx, blk)
        if back:
            store_coefs(mbuf, chunk, 1, idx - 2, total)

    def backward_turn(chunk, idx, front, back):
        total = None
        for blk in range(blk_count):
            if back:
                add = from_points(dh_mat, dpre_buf, blk)
                total = add if total is None else total + add
            if front:
                grad_points(idx, blk)
        if back:
            store_coefs(dhbuf, chunk, 0, idx - 1, total)

    def loop(turn, first, last):
        for idx in range(first, last):
            turn(idx)

    def forward_grid(chunk, between, last):
        full = functools.partial(forward_turn, chunk, front=True, mid=True, back=True)
        split = steps - 4
        forward_turn(chunk, 0, True, False, False)
        forward_turn(chunk, 1, True, True, False)
        loop(full, 2, split)
        between()
        loop(full, split, steps)
        last()
        forward_turn(chunk, steps, False, True, True)
        forward_turn(chunk, steps + 1, False, False, True)
        backward_turn(chunk, 0, True, False)

    def backward_grid(chunk, between, last):
        full = functools.partial(backward_turn, chunk, front=True, back=True)
        split = steps // 2 + 1
        loop(full, 1, split)
        between()
        loop(full, split, steps - 1)
        last()
        full(steps - 1)
        backward_turn(chunk, steps, False, True)

    def down_grads(chunk):
        for degree in range(degrees):
            rows = pl.ds(degree * hidden, hidden)
            wgrad[0][rows, :] += mm_nt(lane_cat(mbuf, chunk, degree), lane_cat(gfull, chunk, degree))

    def up_grads(chunk, half):
        rows = slice(half * hidden // 2, (half + 1) * hidden // 2)
        mats = []
        for degree in range(degrees):
            d_hid = [dhbuf[chunk, coef, rows, :] for coef in degree_span(degree)]
            d_hid = d_hid[0] if len(d_hid) == 1 else jnp.concatenate(d_hid, axis=1)
            mats.append(mm_nt(lane_cat(nfull, chunk, degree), d_hid))
        mats.append(mm_nt(nfull[chunk, 0], dpg_buf[chunk, rows, :]))
        for pair in range(len(mats) // 2):
            wgrad[1 + half][pl.ds(pair * channels, channels), :] += jnp.concatenate(mats[2 * pair:2 * pair + 2], axis=1)

    def store_part(arr, chunk, per_degree):
        for coef, value in enumerate(split_coefs(per_degree)):
            part[arr, chunk, coef] = value.astype(BF16)

    def input_grads(chunk):
        per_degree = [mm(up_ref[degree], lane_cat(dhbuf, chunk, degree)) for degree in range(degrees)]
        per_degree[0] = per_degree[0] + mm(gate_ref[...], dpg_buf[chunk])
        store_part(dxs, chunk, per_degree)

    def outputs(chunk):
        store_part(outs, chunk, [mm(down_t[degree], lane_cat(mbuf, chunk, degree)) for degree in range(degrees)])

    chips = (1 - me // 2, me // 2)

    def scatter_core(arr, chunk):
        for slot, chip in enumerate(chips):
            rows = chan_rows(2 * chip + 1 - me % 2, chan_loc)
            send(('rs1', arr, chunk, slot), part.at[arr, chunk, :, rows, :], rs1.at[arr, chunk, slot],
                 rs1_ss.at[arr, chunk, slot], rs1_rs.at[arr, chunk, slot], 'tp', tp_peer(1))

    def chip_sum(arr, chunk, slot):
        copies[('rs1', arr, chunk, slot)].wait_recv()
        own = part[arr, chunk, :, chan_rows(2 * chips[slot] + me % 2, chan_loc), :].astype(F32)
        return own + rs1[arr, chunk, slot].astype(F32)

    def scatter_chip(arr, chunk):
        rs2_src[arr, chunk] = chip_sum(arr, chunk, 0).astype(BF16)
        send(('rs2', arr, chunk), rs2_src.at[arr, chunk], rs2.at[arr, chunk], rs2_ss.at[arr, chunk], rs2_rs.at[arr, chunk], 'tp', tp_peer(2))

    def scattered(arr, chunk):
        total = chip_sum(arr, chunk, 1)
        copies[('rs2', arr, chunk)].wait_recv()
        return total + rs2[arr, chunk].astype(F32)

    def own_x(chunk):
        return x_ref[:, :, chunk * LANES:(chunk + 1) * LANES].astype(F32)

    def finish_out(chunk):
        out_ref[:, :, chunk * LANES:(chunk + 1) * LANES] = (own_x(chunk) + scattered(outs, chunk)).astype(BF16)

    def own_gain(degree):
        return gain_cols[degree, chan_rows(me, chan_loc), :]

    def back_stats(chunk):
        x_own = own_x(chunk)
        d_norm = rounded(scattered(dxs, chunk))
        rs2[dxs, chunk] = d_norm.astype(BF16)
        d_hat = d_norm[0] * own_gain(0)
        hat = (x_own[0] - stat_buf[chunk, 0:1, :]) * stat_buf[chunk, 1:2, :]
        back_src[chunk, 0:1, :] = jnp.sum(d_hat, axis=0, keepdims=True)
        back_src[chunk, 1:2, :] = jnp.sum(d_hat * hat, axis=0, keepdims=True)
        total = jnp.zeros((chan_loc, LANES), F32)
        for degree in range(1, degrees):
            for coef in degree_span(degree):
                total = total + d_norm[coef] * own_gain(degree) * x_own[coef]
        back_src[chunk, 2:3, :] = jnp.sum(total, axis=0, keepdims=True)
        for hop in (2, 3, 1):
            send(('back', chunk, hop), back_src.at[chunk], back_rx.at[chunk, hop - 1], back_ss.at[chunk, hop - 1], back_rs.at[chunk, hop - 1], 'tp', tp_peer(hop))

    def finish_dx(chunk):
        for hop in (1, 2, 3):
            copies[('back', chunk, hop)].wait_recv()
        sums = (back_src[chunk] + back_rx[chunk, 0]) + (back_rx[chunk, 1] + back_rx[chunk, 2])
        mean, inv_s, inv_v = (stat_buf[chunk, j:j + 1, :] for j in range(3))
        lanes = slice(chunk * LANES, (chunk + 1) * LANES)
        hat = (x_ref[0, :, lanes].astype(F32) - mean) * inv_s
        d_hat = rs2[dxs, chunk, 0].astype(F32) * own_gain(0)
        d_scalar = inv_s * (d_hat - sums[0:1] / channels - hat * (sums[1:2] / channels))
        dx_ref[0, :, lanes] = (d_scalar + g_ref[0, :, lanes].astype(F32)).astype(BF16)
        scale = (inv_v * inv_v * inv_v) * (sums[2:3] / vec_count)
        for degree in range(1, degrees):
            for coef in degree_span(degree):
                d_hat = rs2[dxs, chunk, coef].astype(F32) * own_gain(degree)
                d_vec = inv_v * d_hat - x_ref[coef, :, lanes].astype(F32) * scale
                dx_ref[coef, :, lanes] = (d_vec + g_ref[coef, :, lanes].astype(F32)).astype(BF16)

    def quarter_rows(group, dp):
        quarter = wgrad[group].shape[0] // 4
        return pl.ds(pl.multiple_of(dp * quarter, 16), quarter)

    def wgrad_scatter(group):
        for hop in (3, 1, 2):
            send(('w1', group, hop), wgrad[group].at[quarter_rows(group, dp_peer(hop))], wgrad_rx[group].at[hop - 1],
                 w1_ss.at[group, hop - 1], w1_rs.at[group, hop - 1], 'dp', dp_peer(hop))

    def wgrad_reduce(group):
        for hop in (1, 2, 3):
            copies[('w1', group, hop)].wait_recv()
        mine = quarter_rows(group, my_dp)
        got = wgrad_rx[group]
        total = ((wgrad[group][mine, :] + got[0]) + (got[1] + got[2])).astype(BF16)
        wsum[group][...] = total
        wfull[group][mine, :] = total
        for hop in (3, 1, 2):
            send(('w2', group, hop), wsum[group], wfull[group].at[mine], w2_ss.at[group, hop - 1], w2_rs.at[group, hop - 1], 'dp', dp_peer(hop))

    def wgrad_finish(group):
        for hop in (1, 2, 3):
            copies[('w2', group, hop)].wait_recv()

    def wgrad_store():
        ddown_ref[...] = wfull[0][...]
        for mat in range(degrees + 1):
            rows = slice(mat // 2 * channels, (mat // 2 + 1) * channels)
            lanes = slice(mat % 2 * hidden // 2, (mat % 2 + 1) * hidden // 2)
            value = jnp.concatenate([wfull[1][rows, lanes], wfull[2][rows, lanes]], axis=1)
            if mat < degrees:
                dup_ref[mat * channels:(mat + 1) * channels, :] = value
            else:
                dgate_ref[...] = value

    relay(feat, 0)
    for hop in (1, 2, 3):
        copies[('gain', hop)].wait_recv()
        gain_block(tp_peer(hop), gain_rx[hop - 1])
    gathered(feat, 0)
    normalize(0)
    hidden_part(0)
    def arrived(chunk):
        gathered(grad, chunk)
        grad_part(chunk)

    forward_grid(0, lambda: relay(grad, 0), lambda: arrived(0))
    outputs(0)
    scatter_core(outs, 0)

    def between_a():
        scatter_chip(outs, 0)
        relay(feat, 1)

    def last_a():
        gathered(feat, 1)
        down_grads(0)

    backward_grid(0, between_a, last_a)
    input_grads(0)
    scatter_core(dxs, 0)
    up_grads(0, 0)
    up_grads(0, 1)
    normalize(1)
    scatter_chip(dxs, 0)
    hidden_part(1)
    forward_grid(1, lambda: relay(grad, 1), lambda: arrived(1))
    outputs(1)
    scatter_core(outs, 1)
    down_grads(1)
    wgrad_scatter(0)
    scatter_chip(outs, 1)

    def between_b():
        up_grads(1, 0)
        wgrad_scatter(1)

    backward_grid(1, between_b, lambda: None)
    input_grads(1)
    scatter_core(dxs, 1)
    up_grads(1, 1)
    wgrad_scatter(2)
    scatter_chip(dxs, 1)
    wgrad_reduce(0)
    wgrad_reduce(1)
    back_stats(0)
    finish_out(0)
    finish_out(1)
    wgrad_reduce(2)
    finish_dx(0)
    back_stats(1)
    for group in range(3):
        wgrad_finish(group)
    wgrad_store()
    finish_dx(1)
    for copy in copies.values():
        copy.wait_send()


def hand_on(*refs):
    count = (len(refs) - 2) // 3
    srcs, dsts, bufs, (in_sem, out_sem) = refs[:count], refs[count:2 * count], refs[2 * count:3 * count], refs[3 * count:]
    ins = [pltpu.make_async_copy(srcs[j], bufs[j], in_sem.at[j]) for j in range(count)]
    outs = [pltpu.make_async_copy(bufs[j], dsts[j], out_sem.at[j]) for j in range(count)]
    for copy in ins:
        copy.start()
    for j in range(count):
        ins[j].wait()
        outs[j].start()
    for copy in outs:
        copy.wait()


def solution(mesh):
    act_spec = P('dp', None, 'tp')
    in_specs = (act_spec, P(None, 'tp'), P(None, None, 'tp'), P(None, 'tp'), P(None, 'tp', None), P(None, None), P(None, None), act_spec)
    out_specs = (act_spec, act_spec, P(None, None, 'tp'), P(None, 'tp'), P(None, 'tp', None))

    def local_step(x_loc, gain_loc, up_loc, gate_loc, down_loc, to_grid, from_grid, grad_loc):
        nodes, coefs, chan_loc = x_loc.shape
        degrees, channels, hidden = up_loc.shape
        points = to_grid.shape[1]
        blk_pts = 28
        blks = points // blk_pts
        chunks = nodes // LANES
        groups = hidden // SUB
        w_rows = (degrees * hidden, (degrees + 1) * channels // 2, (degrees + 1) * channels // 2)
        dma = pltpu.SemaphoreType.DMA

        def vm(*shape, dtype=BF16):
            return pltpu.VMEM(shape, dtype)

        full = (chunks, coefs, channels, LANES)
        ins = (x_loc.transpose(1, 2, 0), grad_loc.transpose(1, 2, 0), gain_loc, up_loc, gate_loc, down_loc, to_grid, from_grid.T)
        scratch = [vm(*arr.shape, dtype=arr.dtype) for arr in ins] + [
            dma((len(ins),)), vm(*full), vm(*full), vm(*full),
            vm(3, degrees, chan_loc, dtype=F32), vm(degrees, channels, LANES, dtype=F32),
            vm(degrees, hidden, channels), vm(degrees, channels, hidden), vm(hidden, channels),
            vm(blks, 2, blk_pts * SUB, LANES), vm(blks, 2, blk_pts * SUB, LANES), vm(blks, 2, (coefs - 1) * SUB, LANES), vm(blks, 2, (coefs + 1) * SUB, LANES),
            vm(groups, KPAD, LANES), vm(groups, KPAD, LANES), vm(groups // 2, blks, 2, blk_pts * SUB, LANES, dtype=F32),
            vm(hidden, LANES, dtype=F32), vm(blks, 2, blk_pts * SUB, LANES), vm(blks, 2, blk_pts * SUB, LANES), vm(blks, 2, blk_pts * SUB, LANES), vm(chunks, coefs, hidden, LANES), vm(chunks, coefs, hidden, LANES), vm(chunks, hidden, LANES),
            vm(chunks, SUB, LANES, dtype=F32),
            vm(2, *full), vm(2, chunks, 2, coefs, chan_loc, LANES), vm(2, chunks, coefs, chan_loc, LANES), vm(2, chunks, coefs, chan_loc, LANES),
            vm(chunks, SUB, LANES, dtype=F32), vm(chunks, 3, SUB, LANES, dtype=F32),
            *(vm(rows, LANES, dtype=F32) for rows in w_rows), *(vm(3, rows // 4, LANES, dtype=F32) for rows in w_rows),
            *(vm(rows // 4, LANES) for rows in w_rows), *(vm(rows, LANES) for rows in w_rows),
            dma((2, chunks, 3)), dma((2, chunks, 3)), dma((3,)), dma((3,)),
            dma((2, chunks, 2)), dma((2, chunks, 2)), dma((2, chunks)), dma((2, chunks)),
            dma((chunks, 3)), dma((chunks, 3)), dma((3, 3)), dma((3, 3)), dma((3, 3)), dma((3, 3)),
        ]
        vmem = pl.BlockSpec(memory_space=pltpu.VMEM)
        act = jax.ShapeDtypeStruct((coefs, chan_loc, nodes), BF16)
        shapes = (act, act, jax.ShapeDtypeStruct((degrees * channels, hidden), BF16), jax.ShapeDtypeStruct((channels, hidden), BF16), jax.ShapeDtypeStruct((degrees * hidden, channels), BF16))
        results = pl.pallas_call(
            functools.partial(kernel, {'chunks': chunks, 'blk_pts': blk_pts}),
            out_shape=shapes,
            in_specs=[pl.BlockSpec(memory_space=pl.ANY)] * len(ins),
            out_specs=(vmem,) * 5,
            scratch_shapes=scratch,
            compiler_params=pltpu.CompilerParams(collective_id=0, has_side_effects=True, vmem_limit_bytes=62 * 1024 * 1024),
            name='s2_ffn',
        )(*ins)
        out_t, dx_t, d_up, d_gate, d_down = pl.pallas_call(
            hand_on,
            out_shape=shapes,
            in_specs=[pl.BlockSpec(memory_space=pl.ANY)] * len(shapes),
            out_specs=(pl.BlockSpec(memory_space=pl.ANY),) * len(shapes),
            scratch_shapes=[vm(*arr.shape) for arr in shapes] + [dma((len(shapes),)), dma((len(shapes),))],
            compiler_params=pltpu.CompilerParams(vmem_limit_bytes=62 * 1024 * 1024),
            name='hand_on',
        )(*results)
        return (out_t.transpose(2, 0, 1), dx_t.transpose(2, 0, 1), d_up.reshape(degrees, channels, hidden), d_gate, d_down.reshape(degrees, hidden, channels))

    return jax.shard_map(local_step, mesh=mesh, in_specs=in_specs, out_specs=out_specs, check_vma=False)
```
